32 devices in a mesh: segment: 8 (over z, x), dp: 4 (over y, core).
Axes of the slice: x: 2, y: 2, z: 4, core: 2. Of those that a mesh axis runs over, the one named last changes fastest.
Arguments:
- src_embed: bfloat16 [16, 128, 2048], P('dp', None, 'segment'), parts along dimension 0, may hold values from -6 to 6
- tgt_embed: bfloat16 [16, 128, 2048], P('dp', None, 'segment'), parts along dimension 0, may hold values from -6 to 6
- src_lengths: int32 [16], P('dp'), parts along dimension 0, may hold values from 32 to 128
- tgt_lengths: int32 [16], P('dp'), parts along dimension 0, may hold values from 32 to 128
- attn_in: bfloat16 [8, 2048, 3072], P('segment'), may hold values from -0.125 to 0.125
- attn_out: bfloat16 [8, 1024, 2048], P('segment'), may hold values from -0.375 to 0.375
- norm_gain: float32 [4, 2048], replicated, may hold values from 0.25 to 1.75
- final_gain: float32 [2048], replicated, may hold values from 0.25 to 1.75
Outputs:
- decoded: bfloat16 [16, 128, 2048], P('dp', None, 'segment'), parts along dimension 0
The draws below stay inside these ranges and needn't reach their ends.
There are 4 independent parts, one for each index of `dp`. The reference program is written for one: setup_inputs(seed, part) draws one part's arguments, and reference() takes and returns one part's arrays. A program takes and returns all parts, laid end to end along the dimension named above; an argument that names none is the same for every part. Nothing has to cross between parts.
Inputs may be any that keep to these rules, and one draw needn't show every extreme that they name: `src_lengths`: keys at positions below a sequence's length are its real tokens. `tgt_lengths`: keys at positions below a sequence's length are its real tokens.
All inputs are finite; a program needn't handle non-finite values.
Results may differ from the reference program's by a relative error of at most 0.015.
Values may be sent and summed in bfloat16 or wider, within the bound.
No kernel may reach another device: no remote copies, remote signals or barrier semaphores. Data moves between devices by JAX's collectives and lax.ppermute only.
A program may use at most 64 MiB of HBM per device.

```python
import jax
import jax.numpy as jnp
from jax import lax

D = 2048
HEAD = 64
MB = 4
S = 128
GROUP = 2
INNER = 2048
N_SEGMENT = 8


def place_ends(drawn, key, smallest, top_value):
    shape = drawn.shape
    index_at = [jax.random.randint(jax.random.fold_in(key, axis), (), 0, shape[axis]) for axis in range(len(shape))]
    drawn = drawn.at[tuple(index_at)].set(smallest)
    longest = shape.index(max(shape))
    index_at[longest] = (index_at[longest] + 1) % shape[longest]
    return drawn.at[tuple(index_at)].set(top_value)


def block_levels(stream_key, extent, cuts, low, top_value):
    def one(axis_at, blocks):
        steps = jax.random.uniform(jax.random.fold_in(jax.random.fold_in(stream_key, 6), axis_at), (blocks,), jnp.float32, low / len(cuts), top_value / len(cuts))
        return jnp.repeat(jnp.exp(steps), extent[axis_at] // blocks).reshape((-1,) + (1,) * (len(extent) - axis_at - 1))

    gain = one(*cuts[0])
    for cut in cuts[1:]:
        gain = gain * one(*cut)
    return gain


def centred(own_key, shape, deviation, most, cuts=(), kind=jnp.bfloat16):
    array = jax.random.normal(own_key, shape, jnp.float32) * deviation
    if len(cuts) > 0:
        array = block_levels(own_key, shape, cuts, -0.22, 0.18) * array
    return jnp.clip(array, min=-most, max=most).astype(kind)


def setup_inputs(seed: int = 0, part: int = 0) -> dict:
    key_list = jax.random.split(jax.random.key(seed), 9)
    part_keys = jax.random.split(jax.random.fold_in(key_list[8], part), 9)
    return {
        "src_embed": centred(part_keys[0], (MB, S, D), 1.0, 6.0, ((2, 8),)),
        "tgt_embed": centred(part_keys[1], (MB, S, D), 1.0, 6.0, ((2, 8),)),
        "src_lengths": place_ends(jax.random.randint(part_keys[2], (MB,), S // 4, S + 1), jax.random.fold_in(part_keys[2], 1), S // 4, S).astype(jnp.int32),
        "tgt_lengths": place_ends(jax.random.randint(part_keys[3], (MB,), S // 4, S + 1), jax.random.fold_in(part_keys[3], 1), S // 4, S).astype(jnp.int32),
        "attn_in": centred(key_list[4], (N_SEGMENT, D, 3 * INNER // GROUP), D ** -0.5, 0.125, ((0, 8),)),
        "attn_out": centred(key_list[5], (N_SEGMENT, INNER // GROUP, D), (INNER // 8) ** -0.5, 0.375, ((0, 8),)),
        "norm_gain": jnp.clip(1.0 + 0.15 * jax.random.normal(key_list[6], (4, D), jnp.float32), 0.25, 1.75),
        "final_gain": jnp.clip(1.0 + 0.15 * jax.random.normal(key_list[7], (D,), jnp.float32), 0.25, 1.75),
    }


epsilon = 1e-06
score_scale = 0.125

def rms_scale(values, gain_vector):
    return values * lax.rsqrt(lax.optimization_barrier(jnp.mean(values * values, axis=-1, keepdims=True)) + epsilon) * gain_vector

def attention(queries, key_rows, values, allowed):
    head_count = queries.shape[1] // HEAD
    shaped_q = queries.reshape(queries.shape[0], head_count, HEAD).astype(jnp.float32)
    shaped_k = key_rows.reshape(key_rows.shape[0], head_count, HEAD).astype(jnp.float32)
    shaped_v = values.reshape(values.shape[0], head_count, HEAD).astype(jnp.float32)
    scores = jnp.einsum('qhd,khd->hqk', shaped_q, shaped_k) * score_scale
    scores = jnp.where(allowed[None], scores, -1000000000.0)
    weights = jax.nn.softmax(scores, axis=-1).astype(jnp.bfloat16)
    mixture = jnp.einsum('hqk,khd->qhd', weights.astype(jnp.float32), shaped_v)
    return mixture.reshape(queries.shape[0], -1).astype(jnp.bfloat16)

def sublayer(inputs, memory, attn_in, attn_out, norm_gain, layer_slot, group_size, allowed):
    normed = rms_scale(inputs.astype(jnp.float32), norm_gain[layer_slot]).astype(jnp.bfloat16)
    source = normed if memory is None else memory
    summed = jnp.zeros(inputs.shape, jnp.float32)
    for member in range(group_size):
        weight_slot = layer_slot * group_size + member
        in_weight = attn_in[weight_slot]
        out_weight = attn_out[weight_slot]
        head_cols = out_weight.shape[0]
        queries = jnp.dot(normed, in_weight[:, :head_cols], preferred_element_type=jnp.float32).astype(jnp.bfloat16)
        key_value = jnp.dot(source, in_weight[:, head_cols:], preferred_element_type=jnp.float32).astype(jnp.bfloat16)
        mixture = attention(queries, key_value[:, :head_cols], key_value[:, head_cols:], allowed)
        summed = summed + jnp.dot(mixture, out_weight, preferred_element_type=jnp.float32)
    return (inputs.astype(jnp.float32) + summed).astype(jnp.bfloat16)

def reference(src_embed, tgt_embed, src_lengths, tgt_lengths, attn_in, attn_out, norm_gain, final_gain):
    group_size = N_SEGMENT // 4
    positions = jnp.arange(S, dtype=jnp.int32)
    causal = positions[None, :] <= positions[:, None]
    results = []
    for batch_slot in range(MB):
        source_ok = jnp.broadcast_to(positions[None, :] < src_lengths[batch_slot], (S, S))
        target_ok = (positions[None, :] < tgt_lengths[batch_slot]) & causal
        encoded = src_embed[batch_slot]
        for layer_slot in range(2):
            encoded = sublayer(encoded, None, attn_in, attn_out, norm_gain, layer_slot, group_size, source_ok)
        memory = rms_scale(encoded.astype(jnp.float32), final_gain).astype(jnp.bfloat16)
        decoded = sublayer(tgt_embed[batch_slot], memory, attn_in, attn_out, norm_gain, 2, group_size, source_ok)
        decoded = sublayer(decoded, None, attn_in, attn_out, norm_gain, 3, group_size, target_ok)
        results.append(decoded)
    return jnp.stack(results)
```

```python
import functools

import jax
import jax.numpy as jnp
from jax import lax
from jax.experimental import pallas as pl
from jax.experimental.pallas import tpu as pltpu
from jax.sharding import PartitionSpec as P

HEAD = 64
SECTIONS = 4
CHUNKS = 2
SKEW = 2

epsilon = 1e-06
score_scale = 0.125


VMEM = pl.BlockSpec(memory_space=pltpu.VMEM)
ANY = pl.BlockSpec(memory_space=pl.ANY)
SMEM = pl.BlockSpec(memory_space=pltpu.SMEM)
f32 = jnp.float32
bf16 = jnp.bfloat16


def dot(a, b):
    return jnp.dot(a, b, preferred_element_type=f32)


def column_tile(width):
    return 512 if width % 512 == 0 else width


def params(vmem):
    return pltpu.CompilerParams(vmem_limit_bytes=vmem)


def scaled(x_refs, gain_ref, part, group, share, sections):
    squares = 0.0
    lhs = []
    per = sections // len(x_refs)
    for z in range(sections):
        ref = x_refs[z // per]
        at = (z % per) * share
        x = ref[:, at : at + share].astype(f32)
        squares = squares + jnp.sum(x * x, axis=-1, keepdims=True)
        column = pl.multiple_of((z * group + part) * share, share)
        lhs.append((x * gain_ref[:, pl.ds(column, share)]).astype(bf16))
    return lhs, squares


def rows_of(z, part, group, share):
    return pl.ds(pl.multiple_of((z * group + part) * share, share), share)


def project(lhs_q, lhs_kv, w_ref, parts, group, share, head_cols, emit):
    tile = column_tile(head_cols)
    for start in range(0, 3 * head_cols, tile):
        total = None
        for (part, lq), (_, lk) in zip(zip(parts, lhs_q), zip(parts, lhs_kv)):
            source = lq if start < head_cols else lk
            for z, block in enumerate(source):
                rows = rows_of(z, part, group, share)
                term = dot(block, w_ref[rows, start : start + tile])
                total = term if total is None else total + term
        emit(start, tile, total)


def own_kernel(group, same, scal, after, *refs):
    n = CHUNKS
    xk = refs[:n]
    refs = refs[n:]
    if same:
        xq = xk
    else:
        xq = refs[:n]
        refs = refs[n:]
    gq, gk, w, acc, sums = refs
    head_cols = w.shape[1] // 3
    share = w.shape[0] // (group * SECTIONS)

    @pl.when(scal[1] == 1)
    def _():
        part = scal[0]
        lk, sk = scaled(xk, gk, part, group, share, SECTIONS)
        lq, sq = scaled(xq, gq, part, group, share, SECTIONS)

        def emit(start, tile, total):
            acc[:, start : start + tile] = total

        project([lq], [lk], w, [part], group, share, head_cols, emit)
        sums[:, 0:128] = jnp.broadcast_to(sq, (sq.shape[0], 128))
        sums[:, 128:256] = jnp.broadcast_to(sk, (sk.shape[0], 128))


def rest_kernel(group, same, scal, after, *refs):
    n = CHUNKS * (group - 1)
    xk = refs[:n]
    refs = refs[n:]
    if same:
        xq = xk
    else:
        xq = refs[:n]
        refs = refs[n:]
    gq, gk, w, wo, acc, sums = refs[:6]
    sends = refs[6 : 6 + n]
    mix, qkv = refs[6 + n :]
    head_cols = w.shape[1] // 3
    width = w.shape[0]
    share = width // (group * SECTIONS)
    rows = mix.shape[0]

    @pl.when(scal[1] == 1)
    def _():
        me = scal[0]
        parts, lqs, lks = [], [], []
        sq = sums[:, 0:1]
        sk = sums[:, 128:129]
        for k in range(1, group):
            part = lax.rem(me + group - k, group)
            at = CHUNKS * (k - 1)
            lk, s = scaled(xk[at : at + CHUNKS], gk, part, group, share, SECTIONS)
            sk = sk + s
            lq, s = scaled(xq[at : at + CHUNKS], gq, part, group, share, SECTIONS)
            sq = sq + s
            parts.append(part)
            lqs.append(lq)
            lks.append(lk)
        rq = lax.rsqrt(sq / width + epsilon)
        rk = lax.rsqrt(sk / width + epsilon)

        def emit(start, tile, total):
            scale = rq if start < head_cols else rk
            total = (acc[:, start : start + tile] + total) * scale
            qkv[:, start : start + tile] = total.astype(bf16)

        project(lqs, lks, w, parts, group, share, head_cols, emit)

        query = lax.broadcasted_iota(jnp.int32, (rows, rows), 0)
        key = lax.broadcasted_iota(jnp.int32, (rows, rows), 1)
        allowed = (key < scal[2]) & ((key <= query) | (scal[3] == 0))
        allowed = jnp.concatenate([allowed.astype(f32)] * 2, 0) > 0.5
        lane = lax.broadcasted_iota(jnp.int32, (rows, 2 * HEAD), 1)
        low = lane < HEAD
        zero = jnp.zeros((), bf16)
        for at in range(0, head_cols, 2 * HEAD):
            q = qkv[:, at : at + 2 * HEAD]
            k = qkv[:, head_cols + at : head_cols + at + 2 * HEAD]
            v = qkv[:, 2 * head_cols + at : 2 * head_cols + at + 2 * HEAD]
            both = jnp.concatenate([jnp.where(low, q, zero), jnp.where(low, zero, q)], 0)
            scores = lax.dot_general(
                both, k, (((1,), (1,)), ((), ())), preferred_element_type=f32
            )
            scores = jnp.where(allowed, scores * score_scale, -1000000000.0)
            top = jnp.max(scores, axis=-1, keepdims=True)
            e = jnp.exp(scores - top)
            weights = (e * (1.0 / jnp.sum(e, axis=-1, keepdims=True))).astype(bf16)
            out = dot(weights, v)
            mix[:, at : at + 2 * HEAD] = jnp.where(low, out[:rows], out[rows:]).astype(bf16)

        mixture = mix[...]
        per = SECTIONS // CHUNKS
        for k in range(1, group):
            part = lax.rem(me + k, group)
            for z in range(SECTIONS):
                ref = sends[(k - 1) * CHUNKS + z // per]
                column = rows_of(z, part, group, share)
                at = (z % per) * share
                ref[:, at : at + share] = dot(mixture, wo[:, column]).astype(bf16)


def tail_kernel(group, scal, mix, *refs):
    xq = refs[:CHUNKS]
    wo = refs[CHUNKS]
    bases = refs[CHUNKS + 1 :]
    share = wo.shape[1] // (group * SECTIONS)

    @pl.when(scal[1] == 1)
    def _():
        mixture = mix[...]
        per = SECTIONS // CHUNKS
        for z in range(SECTIONS):
            column = rows_of(z, scal[0], group, share)
            at = (z % per) * share
            res = xq[z // per][:, at : at + share].astype(f32)
            bases[z // per][:, at : at + share] = dot(mixture, wo[:, column]) + res


def hold_weights(w_in, w_out):
    w_in = pltpu.with_memory_space_constraint(w_in, pltpu.VMEM)
    w_out = pltpu.with_memory_space_constraint(w_out, pltpu.VMEM)

    def touch(a_ref, b_ref, out):
        out[...] = jnp.zeros_like(out)

    token = pl.pallas_call(
        touch,
        out_shape=jax.ShapeDtypeStruct((8, 128), f32),
        in_specs=[VMEM, VMEM],
        out_specs=VMEM,
        compiler_params=params(1 << 20),
        name="touch",
    )(w_in, w_out)
    return w_in, w_out, token


def relay(
    src_embed, tgt_embed, src_lengths, tgt_lengths, attn_in, attn_out, norm_gain, final_gain
):
    axis = "segment"
    segments = lax.axis_size(axis)
    group = segments // SECTIONS
    index = lax.axis_index(axis)
    section = index // group
    member = index % group
    batches, rows, share = src_embed.shape
    part_width = SECTIONS * share
    chunk_width = part_width // CHUNKS
    per = SECTIONS // CHUNKS
    w_in = attn_in[0]
    w_out = attn_out[0]
    head_cols = w_out.shape[0]
    gain_q = lax.dynamic_index_in_dim(norm_gain, section, 0, keepdims=True)
    gain_kv = jnp.where(section == 2, final_gain[None], gain_q)

    def permute(value, pairs):
        return lax.ppermute(value, axis, pairs)

    def gather_to(target, value):
        parts = []
        for k in range(group):
            pieces = []
            for z in range(SECTIONS):
                pairs = [
                    (z * group + q, target * group + (q + k) % group) for q in range(group)
                ]
                if z == target and k == 0:
                    pieces.append(value)
                else:
                    pieces.append(permute(value, pairs))
            parts.append(pieces)
        return parts

    def chunks_of(parts):
        return [
            [jnp.concatenate(pieces[c * per : (c + 1) * per], -1) for c in range(CHUNKS)]
            for pieces in parts
        ]

    entry = [gather_to(0, src_embed[b]) for b in range(batches)]
    target_parts = gather_to(2, tgt_embed)
    w_in, w_out, token = hold_weights(w_in, w_out)

    is_target = section == 3
    periods = batches + SKEW * (SECTIONS - 1)
    arrived = {}
    exits = {}

    def flat(lists):
        return [v for inner in lists for v in inner]

    def live_at(t):
        return [p for p in range(SECTIONS) if 0 <= t - SKEW * p < batches]

    def gated(values, gate):
        leaves, tree = jax.tree.flatten(values)
        return jax.tree.unflatten(tree, lax.optimization_barrier((leaves, gate))[0])

    def feed(t, gate):
        slot = jnp.clip(t - SKEW * section, 0, batches - 1)
        active = (t - SKEW * section >= 0) & (t - SKEW * section < batches)
        length = jnp.where(is_target, tgt_lengths[slot], src_lengths[slot])
        scal = jnp.stack(
            [member, active.astype(jnp.int32), length, is_target.astype(jnp.int32)]
        ).astype(jnp.int32)
        xk = arrived.get(t)
        if t < batches:
            first = chunks_of(gated(entry[t], gate))
            if xk is None:
                xk = first
            else:
                xk = [
                    [jnp.where(section == 0, a, c) for a, c in zip(fa, xa)]
                    for fa, xa in zip(first, xk)
                ]
        xq = xk
        if 2 in live_at(t):
            b = t - 2 * SKEW
            target = chunks_of(gated([[p[b] for p in row] for row in target_parts], gate))
            xq = [
                [jnp.where(section == 2, a, c) for a, c in zip(ta, xa)]
                for ta, xa in zip(target, xk)
            ]
        return scal, xk, xq

    def own(fed, after):
        scal, xk, xq = fed
        same = xq is xk
        inputs = list(xk[0]) + ([] if same else list(xq[0]))
        return pl.pallas_call(
            functools.partial(own_kernel, group, same),
            out_shape=(
                jax.ShapeDtypeStruct((rows, 3 * head_cols), f32),
                jax.ShapeDtypeStruct((rows, 256), f32),
            ),
            in_specs=[SMEM, ANY] + [VMEM] * (len(inputs) + 3),
            out_specs=(VMEM, VMEM),
            compiler_params=params(2 << 20),
            cost_estimate=pl.CostEstimate(
                flops=2 * rows * part_width * 3 * head_cols,
                bytes_accessed=1 << 20,
                transcendentals=0,
            ),
            name="own",
        )(scal, after, *inputs, gain_q, gain_kv, w_in)

    n_send = CHUNKS * (group - 1)

    def rest(fed, partial, after):
        scal, xk, xq = fed
        same = xq is xk
        inputs = flat(xk[1:]) + ([] if same else flat(xq[1:]))
        outs = pl.pallas_call(
            functools.partial(rest_kernel, group, same),
            out_shape=tuple(
                [jax.ShapeDtypeStruct((rows, chunk_width), bf16)] * n_send
                + [jax.ShapeDtypeStruct((rows, head_cols), bf16)]
            ),
            in_specs=[SMEM, ANY] + [VMEM] * (len(inputs) + 6),
            out_specs=tuple([VMEM] * (n_send + 1)),
            scratch_shapes=[pltpu.VMEM((rows, 3 * head_cols), bf16)],
            compiler_params=params(4 << 20),
            cost_estimate=pl.CostEstimate(
                flops=4 * rows * part_width * 3 * head_cols,
                bytes_accessed=1 << 20,
                transcendentals=rows * rows * (head_cols // HEAD),
            ),
            name="rest",
        )(scal, after, *inputs, gain_q, gain_kv, w_in, w_out, *partial)
        return outs[:n_send], outs[n_send]

    def tail(fed, mix):
        scal, _, xq = fed
        return pl.pallas_call(
            functools.partial(tail_kernel, group),
            out_shape=tuple([jax.ShapeDtypeStruct((rows, chunk_width), f32)] * CHUNKS),
            in_specs=[SMEM] + [VMEM] * (2 + CHUNKS),
            out_specs=tuple([VMEM] * CHUNKS),
            compiler_params=params(1 << 20),
            cost_estimate=pl.CostEstimate(
                flops=2 * rows * part_width * head_cols, bytes_accessed=1 << 20, transcendentals=0
            ),
            name="tail",
        )(scal, mix, *xq[0], w_out)

    fed = feed(0, token)
    partial = own(fed, token)
    after = token
    for t in range(periods):
        live = live_at(t)
        senders = [p for p in live if p < SECTIONS - 1]
        sends, mix = rest(fed, partial, after)
        taken = [
            [
                permute(
                    sends[(k - 1) * CHUNKS + c],
                    [
                        (p * group + q, p * group + (q + k) % group)
                        for p in live
                        for q in range(group)
                    ],
                )
                for k in range(1, group)
            ]
            for c in range(CHUNKS)
        ]
        bases = tail(fed, mix)
        landed = [[None] * CHUNKS for _ in range(group)]
        finals = []
        for c in range(CHUNKS):
            total = bases[c]
            for v in taken[c] if c == 0 else gated(taken[c], after):
                total = total + v.astype(f32)
            total = total.astype(bf16)
            finals.append(total)
            if senders:
                for k in range(group):
                    pairs = [
                        (p * group + q, (p + 1) * group + (q + k) % group)
                        for p in senders
                        for q in range(group)
                    ]
                    landed[k][c] = permute(total, pairs)
            after = total
            if c == 0 and t + 1 < periods:
                fed = feed(t + 1, total)
                partial = own(fed, total)
                after = partial[1]
        if senders:
            arrived[t + SKEW] = landed
        if SECTIONS - 1 in live:
            result = None
            for z in range(SECTIONS):
                piece = finals[z // per][:, (z % per) * share : (z % per + 1) * share]
                if z < SECTIONS - 1:
                    pairs = [((SECTIONS - 1) * group + q, z * group + q) for q in range(group)]
                    piece = permute(piece, pairs)
                result = piece if result is None else jnp.where(section == z, piece, result)
            exits[t - SKEW * (SECTIONS - 1)] = result
    return jnp.stack([exits[b] for b in range(batches)])


def solution(mesh):
    in_specs = (
        P("dp", None, "segment"),
        P("dp", None, "segment"),
        P("dp"),
        P("dp"),
        P("segment", None, None),
        P("segment", None, None),
        P(),
        P(),
    )
    out_specs = P("dp", None, "segment")
    return jax.shard_map(relay, mesh=mesh, in_specs=in_specs, out_specs=out_specs, check_vma=False)
```

```python
import functools

import jax
import jax.numpy as jnp
from jax import lax
from jax.experimental import pallas as pl
from jax.experimental.pallas import tpu as pltpu
from jax.sharding import PartitionSpec as P

HEAD = 64
SECTIONS = 4
CHUNKS = 1

epsilon = 1e-06
score_scale = 0.125


VMEM = pl.BlockSpec(memory_space=pltpu.VMEM)
ANY = pl.BlockSpec(memory_space=pl.ANY)
SMEM = pl.BlockSpec(memory_space=pltpu.SMEM)
f32 = jnp.float32
bf16 = jnp.bfloat16


def dot(a, b):
    return jnp.dot(a, b, preferred_element_type=f32)


def column_tile(width):
    return 512 if width % 512 == 0 else width


def params(vmem):
    return pltpu.CompilerParams(vmem_limit_bytes=vmem)


def scaled(x_refs, gain_ref, part, group, share, sections):
    squares = 0.0
    lhs = []
    per = sections // len(x_refs)
    for z in range(sections):
        ref = x_refs[z // per]
        at = (z % per) * share
        x = ref[:, at : at + share].astype(f32)
        squares = squares + jnp.sum(x * x, axis=-1, keepdims=True)
        column = pl.multiple_of((z * group + part) * share, share)
        lhs.append((x * gain_ref[:, pl.ds(column, share)]).astype(bf16))
    return lhs, squares


def rows_of(z, part, group, share):
    return pl.ds(pl.multiple_of((z * group + part) * share, share), share)


def project(lhs_q, lhs_kv, w_ref, parts, group, share, head_cols, emit):
    tile = column_tile(head_cols)
    for start in range(0, 3 * head_cols, tile):
        total = None
        for (part, lq), (_, lk) in zip(zip(parts, lhs_q), zip(parts, lhs_kv)):
            source = lq if start < head_cols else lk
            for z, block in enumerate(source):
                rows = rows_of(z, part, group, share)
                term = dot(block, w_ref[rows, start : start + tile])
                total = term if total is None else total + term
        emit(start, tile, total)


def own_kernel(group, same, t, table, after, *refs):
    scal = [table[t, i] for i in range(4)]
    n = CHUNKS
    xk = refs[:n]
    refs = refs[n:]
    if same:
        xq = xk
    else:
        xq = refs[:n]
        refs = refs[n:]
    gq, gk, w, acc, sums = refs
    head_cols = w.shape[1] // 3
    share = w.shape[0] // (group * SECTIONS)

    @pl.when(scal[1] == 1)
    def _():
        part = scal[0]
        lk, sk = scaled(xk, gk, part, group, share, SECTIONS)
        lq, sq = scaled(xq, gq, part, group, share, SECTIONS)

        def emit(start, tile, total):
            acc[:, start : start + tile] = total

        project([lq], [lk], w, [part], group, share, head_cols, emit)
        sums[:, 0:128] = jnp.broadcast_to(sq, (sq.shape[0], 128))
        sums[:, 128:256] = jnp.broadcast_to(sk, (sk.shape[0], 128))


def rest_kernel(group, same, t, table, after, *refs):
    scal = [table[t, i] for i in range(4)]
    n = CHUNKS * (group - 1)
    xk = refs[:n]
    refs = refs[n:]
    if same:
        xq = xk
    else:
        xq = refs[:n]
        refs = refs[n:]
    gq, gk, w, wo, acc, sums = refs[:6]
    sends = refs[6 : 6 + n]
    mix, qkv = refs[6 + n :]
    head_cols = w.shape[1] // 3
    width = w.shape[0]
    share = width // (group * SECTIONS)
    rows = mix.shape[0]

    @pl.when(scal[1] == 1)
    def _():
        me = scal[0]
        parts, lqs, lks = [], [], []
        sq = sums[:, 0:1]
        sk = sums[:, 128:129]
        for k in range(1, group):
            part = lax.rem(me + group - k, group)
            at = CHUNKS * (k - 1)
            lk, s = scaled(xk[at : at + CHUNKS], gk, part, group, share, SECTIONS)
            sk = sk + s
            lq, s = scaled(xq[at : at + CHUNKS], gq, part, group, share, SECTIONS)
            sq = sq + s
            parts.append(part)
            lqs.append(lq)
            lks.append(lk)
        rq = lax.rsqrt(sq / width + epsilon)
        rk = lax.rsqrt(sk / width + epsilon)

        def emit(start, tile, total):
            scale = rq if start < head_cols else rk
            total = (acc[:, start : start + tile] + total) * scale
            qkv[:, start : start + tile] = total.astype(bf16)

        project(lqs, lks, w, parts, group, share, head_cols, emit)

        query = lax.broadcasted_iota(jnp.int32, (rows, rows), 0)
        key = lax.broadcasted_iota(jnp.int32, (rows, rows), 1)
        allowed = (key < scal[2]) & ((key <= query) | (scal[3] == 0))
        allowed = jnp.concatenate([allowed.astype(f32)] * 2, 0) > 0.5
        lane = lax.broadcasted_iota(jnp.int32, (rows, 2 * HEAD), 1)
        low = lane < HEAD
        zero = jnp.zeros((), bf16)
        for at in range(0, head_cols, 2 * HEAD):
            q = qkv[:, at : at + 2 * HEAD]
            k = qkv[:, head_cols + at : head_cols + at + 2 * HEAD]
            v = qkv[:, 2 * head_cols + at : 2 * head_cols + at + 2 * HEAD]
            both = jnp.concatenate([jnp.where(low, q, zero), jnp.where(low, zero, q)], 0)
            scores = lax.dot_general(
                both, k, (((1,), (1,)), ((), ())), preferred_element_type=f32
            )
            scores = jnp.where(allowed, scores * score_scale, -1000000000.0)
            top = jnp.max(scores, axis=-1, keepdims=True)
            e = jnp.exp(scores - top)
            weights = (e * (1.0 / jnp.sum(e, axis=-1, keepdims=True))).astype(bf16)
            out = dot(weights, v)
            mix[:, at : at + 2 * HEAD] = jnp.where(low, out[:rows], out[rows:]).astype(bf16)

        mixture = mix[...]
        per = SECTIONS // CHUNKS
        for k in range(1, group):
            part = lax.rem(me + k, group)
            for z in range(SECTIONS):
                ref = sends[(k - 1) * CHUNKS + z // per]
                column = rows_of(z, part, group, share)
                at = (z % per) * share
                ref[:, at : at + share] = dot(mixture, wo[:, column]).astype(bf16)


def tail_kernel(group, t, table, mix, *refs):
    scal = [table[t, i] for i in range(4)]
    xq = refs[:CHUNKS]
    wo = refs[CHUNKS]
    bases = refs[CHUNKS + 1 :]
    share = wo.shape[1] // (group * SECTIONS)

    @pl.when(scal[1] == 1)
    def _():
        mixture = mix[...]
        per = SECTIONS // CHUNKS
        for z in range(SECTIONS):
            column = rows_of(z, scal[0], group, share)
            at = (z % per) * share
            res = xq[z // per][:, at : at + share].astype(f32)
            bases[z // per][:, at : at + share] = dot(mixture, wo[:, column]) + res


def hold_weights(w_in, w_out):
    w_in = pltpu.with_memory_space_constraint(w_in, pltpu.VMEM)
    w_out = pltpu.with_memory_space_constraint(w_out, pltpu.VMEM)

    def touch(a_ref, b_ref, out):
        out[...] = jnp.zeros_like(out)

    token = pl.pallas_call(
        touch,
        out_shape=jax.ShapeDtypeStruct((8, 128), f32),
        in_specs=[VMEM, VMEM],
        out_specs=VMEM,
        compiler_params=params(1 << 20),
        name="touch",
    )(w_in, w_out)
    return w_in, w_out, token


def relay(
    src_embed, tgt_embed, src_lengths, tgt_lengths, attn_in, attn_out, norm_gain, final_gain
):
    axis = "segment"
    segments = lax.axis_size(axis)
    group = segments // SECTIONS
    index = lax.axis_index(axis)
    section = index // group
    member = index % group
    batches, rows, share = src_embed.shape
    part_width = SECTIONS * share
    chunk_width = part_width // CHUNKS
    w_in = attn_in[0]
    w_out = attn_out[0]
    head_cols = w_out.shape[0]
    gain_q = lax.dynamic_index_in_dim(norm_gain, section, 0, keepdims=True)
    gain_kv = jnp.where(section == 2, final_gain[None], gain_q)

    def permute(value, pairs):
        return lax.ppermute(value, axis, pairs)

    def partners(k):
        return [
            (p * group + q, p * group + (q + k) % group)
            for p in range(SECTIONS)
            for q in range(group)
        ]

    def onward(k):
        return [
            (p * group + q, (p + 1) * group + (q + k) % group)
            for p in range(SECTIONS - 1)
            for q in range(group)
        ]

    def shift_pairs(by):
        return [
            (((0 if first else 2) + by) % SECTIONS * group + q, (0 if first else 2) * group + q)
            for first in (True, False)
            for q in range(group)
        ]

    def collect(low, high):
        source = src_embed[low:high]
        target = tgt_embed[low:high]
        payloads = [jnp.where(section == by, source, target) for by in range(SECTIONS)]
        payloads = lax.optimization_barrier(payloads)
        pieces = {0: payloads[0]}
        for by in range(1, SECTIONS):
            pieces[by] = permute(payloads[by], shift_pairs(by))
        return pieces

    def part_of(pieces, at):
        rotated = [pieces[by][at] for by in range(SECTIONS)]
        ordered = []
        for z in range(SECTIONS):
            value = rotated[z]
            other = rotated[(z - 2) % SECTIONS]
            ordered.append(jnp.where(section == 0, value, other))
        width = chunk_width // share
        return [
            jnp.concatenate(ordered[c * width : (c + 1) * width], -1) for c in range(CHUNKS)
        ]

    periods = batches + SECTIONS - 1
    step = jnp.arange(periods, dtype=jnp.int32)
    slot = step - section
    lengths = jnp.where(section == SECTIONS - 1, tgt_lengths, src_lengths)
    here = slot[:, None] == jnp.arange(batches, dtype=jnp.int32)[None]
    table = jnp.stack(
        [
            jnp.broadcast_to(member, step.shape),
            jnp.any(here, axis=1).astype(jnp.int32),
            jnp.sum(jnp.where(here, lengths[None], 0), axis=1),
            jnp.broadcast_to((section == SECTIONS - 1).astype(jnp.int32), step.shape),
        ],
        axis=1,
    ).astype(jnp.int32)

    early = collect(0, 1)
    late = collect(1, batches)
    w_in, w_out, token = hold_weights(w_in, w_out)
    entry = {}

    def enter(b):
        mine = part_of(early, 0) if b == 0 else part_of(late, b - 1)
        parts = [mine]
        for k in range(1, group):
            parts.append([permute(v, partners(k)) for v in mine])
        entry[b] = parts


    def flat(lists):
        return [v for inner in lists for v in inner]

    def feed(t, came):
        def merge(at, ours, theirs):
            return [
                [jnp.where(section == at, a, c) for a, c in zip(ra, rc)]
                for ra, rc in zip(ours, theirs)
            ]

        xk = came
        if t < batches:
            xk = entry[t] if came is None else merge(0, entry[t], came)
        xq = xk
        if 0 <= t - 2 < batches:
            xq = merge(2, entry[t - 2], xk)
        return t, xk, xq

    def own(fed, after):
        t, xk, xq = fed
        same = xq is xk
        inputs = list(xk[0]) + ([] if same else list(xq[0]))
        return pl.pallas_call(
            functools.partial(own_kernel, group, same, t),
            out_shape=(
                jax.ShapeDtypeStruct((rows, 3 * head_cols), f32),
                jax.ShapeDtypeStruct((rows, 256), f32),
            ),
            in_specs=[SMEM, ANY] + [VMEM] * (len(inputs) + 3),
            out_specs=(VMEM, VMEM),
            compiler_params=params(2 << 20),
            cost_estimate=pl.CostEstimate(
                flops=2 * rows * part_width * 3 * head_cols,
                bytes_accessed=1 << 20,
                transcendentals=0,
            ),
            name="own",
        )(table, after, *inputs, gain_q, gain_kv, w_in)

    n_send = CHUNKS * (group - 1)

    def rest(fed, partial, after):
        t, xk, xq = fed
        same = xq is xk
        inputs = flat(xk[1:]) + ([] if same else flat(xq[1:]))
        outs = pl.pallas_call(
            functools.partial(rest_kernel, group, same, t),
            out_shape=tuple(
                [jax.ShapeDtypeStruct((rows, chunk_width), bf16)] * n_send
                + [jax.ShapeDtypeStruct((rows, head_cols), bf16)]
            ),
            in_specs=[SMEM, ANY] + [VMEM] * (len(inputs) + 6),
            out_specs=tuple([VMEM] * (n_send + 1)),
            scratch_shapes=[pltpu.VMEM((rows, 3 * head_cols), bf16)],
            compiler_params=params(4 << 20),
            cost_estimate=pl.CostEstimate(
                flops=4 * rows * part_width * 3 * head_cols,
                bytes_accessed=1 << 20,
                transcendentals=rows * rows * (head_cols // HEAD),
            ),
            name="rest",
        )(table, after, *inputs, gain_q, gain_kv, w_in, w_out, *partial)
        return outs[:n_send], outs[n_send]

    def tail(fed, mix):
        t, _, xq = fed
        return pl.pallas_call(
            functools.partial(tail_kernel, group, t),
            out_shape=tuple([jax.ShapeDtypeStruct((rows, chunk_width), f32)] * CHUNKS),
            in_specs=[SMEM] + [VMEM] * (2 + CHUNKS),
            out_specs=tuple([VMEM] * CHUNKS),
            compiler_params=params(1 << 20),
            cost_estimate=pl.CostEstimate(
                flops=2 * rows * part_width * head_cols, bytes_accessed=1 << 20, transcendentals=0
            ),
            name="tail",
        )(table, mix, *xq[0], w_out)

    enter(0)
    fed = feed(0, None)
    finals = {}
    exits = {}

    def leave(b):
        value = finals[b]
        pieces = []
        for z in range(SECTIONS):
            at, offset = divmod(z * share, chunk_width)
            piece = value[at][:, offset : offset + share]
            if z < SECTIONS - 1:
                pairs = [((SECTIONS - 1) * group + q, z * group + q) for q in range(group)]
                piece = permute(piece, pairs)
            pieces.append(piece)
        result = pieces[-1]
        for z in range(SECTIONS - 1):
            result = jnp.where(section == z, pieces[z], result)
        exits[b] = result

    for t in range(periods):
        partial = own(fed, token)
        sends, mix = rest(fed, partial, token)
        bases = tail(fed, mix)
        taken = [
            [permute(sends[(k - 1) * CHUNKS + c], partners(k)) for k in range(1, group)]
            for c in range(CHUNKS)
        ]
        if t + 1 < batches:
            enter(t + 1)
        if t - SECTIONS in finals:
            leave(t - SECTIONS)
        came = [[None] * CHUNKS for _ in range(group)]
        done = []
        for c in range(CHUNKS):
            total = bases[c]
            for v in taken[c]:
                total = total + v.astype(f32)
            total = total.astype(bf16)
            done.append(total)
            if t + 1 < periods:
                for k in range(group):
                    came[k][c] = permute(total, onward(k))
        if t >= SECTIONS - 1:
            finals[t - SECTIONS + 1] = done
        if t + 1 < periods:
            fed = feed(t + 1, came)
    leave(batches - 1)
    return jnp.stack([exits[b] for b in range(batches)])


def solution(mesh):
    in_specs = (
        P("dp", None, "segment"),
        P("dp", None, "segment"),
        P("dp"),
        P("dp"),
        P("segment", None, None),
        P("segment", None, None),
        P(),
        P(),
    )
    out_specs = P("dp", None, "segment")
    return jax.shard_map(relay, mesh=mesh, in_specs=in_specs, out_specs=out_specs, check_vma=False)
```

```python
import functools

import jax
import jax.numpy as jnp
from jax import lax
from jax.experimental import pallas as pl
from jax.experimental.pallas import tpu as pltpu
from jax.sharding import PartitionSpec as P

HEAD = 64
SECTIONS = 4
CHUNKS = 1

epsilon = 1e-06
score_scale = 0.125


VMEM = pl.BlockSpec(memory_space=pltpu.VMEM)
ANY = pl.BlockSpec(memory_space=pl.ANY)
SMEM = pl.BlockSpec(memory_space=pltpu.SMEM)
f32 = jnp.float32
bf16 = jnp.bfloat16


def dot(a, b):
    return jnp.dot(a, b, preferred_element_type=f32)


def column_tile(width):
    return 512 if width % 512 == 0 else width


def params(vmem):
    return pltpu.CompilerParams(vmem_limit_bytes=vmem)


def scaled(x_refs, gain_ref, part, group, share, sections):
    squares = 0.0
    lhs = []
    per = sections // len(x_refs)
    for z in range(sections):
        ref = x_refs[z // per]
        at = (z % per) * share
        x = ref[:, at : at + share].astype(f32)
        squares = squares + jnp.sum(x * x, axis=-1, keepdims=True)
        column = pl.multiple_of((z * group + part) * share, share)
        lhs.append((x * gain_ref[:, pl.ds(column, share)]).astype(bf16))
    return lhs, squares


def rows_of(z, part, group, share):
    return pl.ds(pl.multiple_of((z * group + part) * share, share), share)


def project(lhs_q, lhs_kv, w_ref, parts, group, share, head_cols, emit):
    tile = column_tile(head_cols)
    for start in range(0, 3 * head_cols, tile):
        total = None
        for (part, lq), (_, lk) in zip(zip(parts, lhs_q), zip(parts, lhs_kv)):
            source = lq if start < head_cols else lk
            for z, block in enumerate(source):
                rows = rows_of(z, part, group, share)
                term = dot(block, w_ref[rows, start : start + tile])
                total = term if total is None else total + term
        emit(start, tile, total)


def own_kernel(group, same, t, table, after, *refs):
    scal = [table[t, i] for i in range(4)]
    n = CHUNKS
    xk = refs[:n]
    refs = refs[n:]
    if same:
        xq = xk
    else:
        xq = refs[:n]
        refs = refs[n:]
    gq, gk, w, acc, sums = refs
    head_cols = w.shape[1] // 3
    share = w.shape[0] // (group * SECTIONS)

    @pl.when(scal[1] == 1)
    def _():
        part = scal[0]
        lk, sk = scaled(xk, gk, part, group, share, SECTIONS)
        lq, sq = scaled(xq, gq, part, group, share, SECTIONS)

        def emit(start, tile, total):
            acc[:, start : start + tile] = total

        project([lq], [lk], w, [part], group, share, head_cols, emit)
        sums[:, 0:128] = jnp.broadcast_to(sq, (sq.shape[0], 128))
        sums[:, 128:256] = jnp.broadcast_to(sk, (sk.shape[0], 128))


def rest_kernel(group, same, t, table, after, *refs):
    scal = [table[t, i] for i in range(4)]
    n = CHUNKS * (group - 1)
    xk = refs[:n]
    refs = refs[n:]
    if same:
        xq = xk
    else:
        xq = refs[:n]
        refs = refs[n:]
    gq, gk, w, wo, acc, sums = refs[:6]
    sends = refs[6 : 6 + n]
    mix, qkv = refs[6 + n :]
    head_cols = w.shape[1] // 3
    width = w.shape[0]
    share = width // (group * SECTIONS)
    rows = mix.shape[0]

    @pl.when(scal[1] == 1)
    def _():
        me = scal[0]
        parts, lqs, lks = [], [], []
        sq = sums[:, 0:1]
        sk = sums[:, 128:129]
        for k in range(1, group):
            part = lax.rem(me + group - k, group)
            at = CHUNKS * (k - 1)
            lk, s = scaled(xk[at : at + CHUNKS], gk, part, group, share, SECTIONS)
            sk = sk + s
            lq, s = scaled(xq[at : at + CHUNKS], gq, part, group, share, SECTIONS)
            sq = sq + s
            parts.append(part)
            lqs.append(lq)
            lks.append(lk)
        rq = lax.rsqrt(sq / width + epsilon)
        rk = lax.rsqrt(sk / width + epsilon)

        def emit(start, tile, total):
            scale = rq if start < head_cols else rk
            total = (acc[:, start : start + tile] + total) * scale
            qkv[:, start : start + tile] = total.astype(bf16)

        project(lqs, lks, w, parts, group, share, head_cols, emit)

        query = lax.broadcasted_iota(jnp.int32, (rows, rows), 0)
        key = lax.broadcasted_iota(jnp.int32, (rows, rows), 1)
        allowed = (key < scal[2]) & ((key <= query) | (scal[3] == 0))
        allowed = jnp.concatenate([allowed.astype(f32)] * 2, 0) > 0.5
        lane = lax.broadcasted_iota(jnp.int32, (rows, 2 * HEAD), 1)
        low = lane < HEAD
        zero = jnp.zeros((), bf16)
        for at in range(0, head_cols, 2 * HEAD):
            q = qkv[:, at : at + 2 * HEAD]
            k = qkv[:, head_cols + at : head_cols + at + 2 * HEAD]
            v = qkv[:, 2 * head_cols + at : 2 * head_cols + at + 2 * HEAD]
            both = jnp.concatenate([jnp.where(low, q, zero), jnp.where(low, zero, q)], 0)
            scores = lax.dot_general(
                both, k, (((1,), (1,)), ((), ())), preferred_element_type=f32
            )
            scores = jnp.where(allowed, scores * score_scale, -1000000000.0)
            top = jnp.max(scores, axis=-1, keepdims=True)
            e = jnp.exp(scores - top)
            weights = (e * (1.0 / jnp.sum(e, axis=-1, keepdims=True))).astype(bf16)
            out = dot(weights, v)
            mix[:, at : at + 2 * HEAD] = jnp.where(low, out[:rows], out[rows:]).astype(bf16)

        mixture = mix[...]
        per = SECTIONS // CHUNKS
        for k in range(1, group):
            part = lax.rem(me + k, group)
            for z in range(SECTIONS):
                ref = sends[(k - 1) * CHUNKS + z // per]
                column = rows_of(z, part, group, share)
                at = (z % per) * share
                ref[:, at : at + share] = dot(mixture, wo[:, column]).astype(bf16)


def tail_kernel(group, t, table, mix, *refs):
    scal = [table[t, i] for i in range(4)]
    xq = refs[:CHUNKS]
    wo = refs[CHUNKS]
    bases = refs[CHUNKS + 1 :]
    share = wo.shape[1] // (group * SECTIONS)

    @pl.when(scal[1] == 1)
    def _():
        mixture = mix[...]
        per = SECTIONS // CHUNKS
        for z in range(SECTIONS):
            column = rows_of(z, scal[0], group, share)
            at = (z % per) * share
            res = xq[z // per][:, at : at + share].astype(f32)
            bases[z // per][:, at : at + share] = dot(mixture, wo[:, column]) + res


def hold_weights(w_in, w_out):
    w_in = pltpu.with_memory_space_constraint(w_in, pltpu.VMEM)
    w_out = pltpu.with_memory_space_constraint(w_out, pltpu.VMEM)

    def touch(a_ref, b_ref, out):
        out[...] = jnp.zeros_like(out)

    token = pl.pallas_call(
        touch,
        out_shape=jax.ShapeDtypeStruct((8, 128), f32),
        in_specs=[VMEM, VMEM],
        out_specs=VMEM,
        compiler_params=params(1 << 20),
        name="touch",
    )(w_in, w_out)
    return w_in, w_out, token


def relay(
    src_embed, tgt_embed, src_lengths, tgt_lengths, attn_in, attn_out, norm_gain, final_gain
):
    axis = "segment"
    segments = lax.axis_size(axis)
    group = segments // SECTIONS
    index = lax.axis_index(axis).astype(jnp.uint32)
    section = lax.div(index, jnp.uint32(group)).astype(jnp.int32)
    member = lax.rem(index, jnp.uint32(group)).astype(jnp.int32)
    at_section = [section == p for p in range(SECTIONS)]
    section, member, at_section = lax.optimization_barrier((section, member, at_section))
    batches, rows, share = src_embed.shape
    part_width = SECTIONS * share
    chunk_width = part_width // CHUNKS
    w_in = attn_in[0]
    w_out = attn_out[0]
    head_cols = w_out.shape[0]
    gain_q = norm_gain[:1]
    for p in range(1, SECTIONS):
        gain_q = jnp.where(at_section[p], norm_gain[p : p + 1], gain_q)
    gain_kv = jnp.where(at_section[2], final_gain[None], gain_q)

    def permute(value, pairs):
        return lax.ppermute(value, axis, pairs)

    def partners(k):
        return [
            (p * group + q, p * group + (q + k) % group)
            for p in range(SECTIONS)
            for q in range(group)
        ]

    def onward(k):
        return [
            (p * group + q, (p + 1) * group + (q + k) % group)
            for p in range(SECTIONS - 1)
            for q in range(group)
        ]

    def shift_pairs(by):
        return [
            (((0 if first else 2) + by) % SECTIONS * group + q, (0 if first else 2) * group + q)
            for first in (True, False)
            for q in range(group)
        ]

    def collect(low, high):
        source = src_embed[low:high]
        target = tgt_embed[low:high]
        payloads = [jnp.where(at_section[by], source, target) for by in range(SECTIONS)]
        payloads = lax.optimization_barrier(payloads)
        pieces = {0: payloads[0]}
        for by in range(1, SECTIONS):
            pieces[by] = permute(payloads[by], shift_pairs(by))
        return pieces

    def part_of(pieces, at):
        rotated = [pieces[by][at] for by in range(SECTIONS)]
        ordered = []
        for z in range(SECTIONS):
            value = rotated[z]
            other = rotated[(z - 2) % SECTIONS]
            ordered.append(jnp.where(at_section[0], value, other))
        width = chunk_width // share
        return [
            jnp.concatenate(ordered[c * width : (c + 1) * width], -1) for c in range(CHUNKS)
        ]

    periods = batches + SECTIONS - 1
    step = jnp.arange(periods, dtype=jnp.int32)
    slot = step - section
    lengths = jnp.where(at_section[SECTIONS - 1], tgt_lengths, src_lengths)
    here = slot[:, None] == jnp.arange(batches, dtype=jnp.int32)[None]
    table = jnp.stack(
        [
            jnp.broadcast_to(member, step.shape),
            jnp.any(here, axis=1).astype(jnp.int32),
            jnp.sum(jnp.where(here, lengths[None], 0), axis=1),
            jnp.where(at_section[SECTIONS - 1], jnp.ones_like(step), 0),
        ],
        axis=1,
    ).astype(jnp.int32)
    table = pltpu.with_memory_space_constraint(table, pltpu.SMEM)

    early = collect(0, 1)
    late = [collect(1, batches)]
    w_in, w_out, token = hold_weights(w_in, w_out)
    entry = {}

    def enter(b):
        mine = part_of(early, 0) if b == 0 else part_of(late[0], b - 1)
        mine = lax.optimization_barrier(mine)
        parts = [mine]
        for k in range(1, group):
            parts.append([permute(v, partners(k)) for v in mine])
        entry[b] = parts


    def flat(lists):
        return [v for inner in lists for v in inner]

    def gated(values, gate):
        return lax.optimization_barrier((values, gate))[0]

    def merge(at, ours, theirs):
        return [
            [jnp.where(at_section[at], a, c) for a, c in zip(ra, rc)]
            for ra, rc in zip(ours, theirs)
        ]

    def feed(t, came):
        def select(rows):
            xk = None if came is None else came[rows]
            if t < batches:
                mine = entry[t][rows]
                xk = mine if xk is None else merge(0, mine, xk)
            xq = xk
            if 0 <= t - 2 < batches:
                xq = merge(2, entry[t - 2][rows], xk)
            return xk, xq

        xk, xq = select(slice(0, 1))
        partial = own((t, xk, xq), token)
        if came is not None:
            came = came[:1] + gated(came[1:], partial[1])
        more_k, more_q = select(slice(1, None))
        same = xq is xk
        xk = xk + more_k
        return (t, xk, xk if same else xq + more_q), partial

    def own(fed, after):
        t, xk, xq = fed
        same = xq is xk
        inputs = list(xk[0]) + ([] if same else list(xq[0]))
        return pl.pallas_call(
            functools.partial(own_kernel, group, same, t),
            out_shape=(
                jax.ShapeDtypeStruct((rows, 3 * head_cols), f32),
                jax.ShapeDtypeStruct((rows, 256), f32),
            ),
            in_specs=[SMEM, ANY] + [VMEM] * (len(inputs) + 3),
            out_specs=(VMEM, VMEM),
            compiler_params=params(2 << 20),
            cost_estimate=pl.CostEstimate(
                flops=2 * rows * part_width * 3 * head_cols,
                bytes_accessed=1 << 20,
                transcendentals=0,
            ),
            name="own",
        )(table, after, *inputs, gain_q, gain_kv, w_in)

    n_send = CHUNKS * (group - 1)

    def rest(fed, partial, after):
        t, xk, xq = fed
        same = xq is xk
        inputs = flat(xk[1:]) + ([] if same else flat(xq[1:]))
        outs = pl.pallas_call(
            functools.partial(rest_kernel, group, same, t),
            out_shape=tuple(
                [jax.ShapeDtypeStruct((rows, chunk_width), bf16)] * n_send
                + [jax.ShapeDtypeStruct((rows, head_cols), bf16)]
            ),
            in_specs=[SMEM, ANY] + [VMEM] * (len(inputs) + 6),
            out_specs=tuple([VMEM] * (n_send + 1)),
            scratch_shapes=[pltpu.VMEM((rows, 3 * head_cols), bf16)],
            compiler_params=params(4 << 20),
            cost_estimate=pl.CostEstimate(
                flops=4 * rows * part_width * 3 * head_cols,
                bytes_accessed=1 << 20,
                transcendentals=rows * rows * (head_cols // HEAD),
            ),
            name="rest",
        )(table, after, *inputs, gain_q, gain_kv, w_in, w_out, *partial)
        return outs[:n_send], outs[n_send]

    def tail(fed, mix):
        t, _, xq = fed
        return pl.pallas_call(
            functools.partial(tail_kernel, group, t),
            out_shape=tuple([jax.ShapeDtypeStruct((rows, chunk_width), f32)] * CHUNKS),
            in_specs=[SMEM] + [VMEM] * (2 + CHUNKS),
            out_specs=tuple([VMEM] * CHUNKS),
            compiler_params=params(1 << 20),
            cost_estimate=pl.CostEstimate(
                flops=2 * rows * part_width * head_cols, bytes_accessed=1 << 20, transcendentals=0
            ),
            name="tail",
        )(table, mix, *xq[0], w_out)

    enter(0)
    fed, partial = feed(0, None)
    finals = {}
    exits = {}

    def leave(b):
        value = finals[b]
        pieces = []
        for z in range(SECTIONS):
            at, offset = divmod(z * share, chunk_width)
            piece = value[at][:, offset : offset + share]
            if z < SECTIONS - 1:
                pairs = [((SECTIONS - 1) * group + q, z * group + q) for q in range(group)]
                piece = permute(piece, pairs)
            pieces.append(piece)
        result = pieces[-1]
        for z in range(SECTIONS - 1):
            result = jnp.where(at_section[z], pieces[z], result)
        exits[b] = result

    for t in range(periods):
        sends, mix = rest(fed, partial, token)
        bases = tail(fed, mix)
        taken = [
            [permute(sends[(k - 1) * CHUNKS + c], partners(k)) for k in range(1, group)]
            for c in range(CHUNKS)
        ]
        if 0 < t < batches - 1:
            enter(t + 1)
        if t - SECTIONS in finals:
            leave(t - SECTIONS)
        came = [[None] * CHUNKS for _ in range(group)]
        done = []
        for c in range(CHUNKS):
            total = bases[c]
            for v in taken[c]:
                total = total + v.astype(f32)
            total = total.astype(bf16)
            done.append(total)
            if t + 1 < periods:
                for k in range(group):
                    came[k][c] = permute(total, onward(k))
        if t == 0:
            late[0] = gated(late[0], done)
            enter(1)
        if t >= SECTIONS - 1:
            finals[t - SECTIONS + 1] = done
        if t + 1 < periods:
            fed, partial = feed(t + 1, came)
    leave(batches - 1)
    return jnp.stack([exits[b] for b in range(batches)])


def solution(mesh):
    in_specs = (
        P("dp", None, "segment"),
        P("dp", None, "segment"),
        P("dp"),
        P("dp"),
        P("segment", None, None),
        P("segment", None, None),
        P(),
        P(),
    )
    out_specs = P("dp", None, "segment")
    return jax.shard_map(relay, mesh=mesh, in_specs=in_specs, out_specs=out_specs, check_vma=False)
```

```python
import functools

import jax
import jax.numpy as jnp
from jax import lax
from jax.experimental import pallas as pl
from jax.experimental.pallas import tpu as pltpu
from jax.sharding import PartitionSpec as P

HEAD = 64
SECTIONS = 4
CHUNKS = 1

epsilon = 1e-06
score_scale = 0.125


VMEM = pl.BlockSpec(memory_space=pltpu.VMEM)
ANY = pl.BlockSpec(memory_space=pl.ANY)
f32 = jnp.float32
bf16 = jnp.bfloat16


def dot(a, b):
    return jnp.dot(a, b, preferred_element_type=f32)


def column_tile(width):
    return 512 if width % 512 == 0 else width


def params(vmem):
    return pltpu.CompilerParams(vmem_limit_bytes=vmem)


def scaled(x_refs, gain_ref, part, group, share, sections):
    squares = 0.0
    lhs = []
    per = sections // len(x_refs)
    for z in range(sections):
        ref = x_refs[z // per]
        at = (z % per) * share
        x = ref[:, at : at + share].astype(f32)
        squares = squares + jnp.sum(x * x, axis=-1, keepdims=True)
        column = pl.multiple_of((z * group + part) * share, share)
        lhs.append((x * gain_ref[:, pl.ds(column, share)]).astype(bf16))
    return lhs, squares


def rows_of(z, part, group, share):
    return pl.ds(pl.multiple_of((z * group + part) * share, share), share)


def project(lhs_q, lhs_kv, w_ref, parts, group, share, head_cols, emit):
    tile = column_tile(head_cols)
    for start in range(0, 3 * head_cols, tile):
        total = None
        for (part, lq), (_, lk) in zip(zip(parts, lhs_q), zip(parts, lhs_kv)):
            source = lq if start < head_cols else lk
            for z, block in enumerate(source):
                rows = rows_of(z, part, group, share)
                term = dot(block, w_ref[rows, start : start + tile])
                total = term if total is None else total + term
        emit(start, tile, total)


def position(group, t, batches):
    index = lax.axis_index("segment")
    section = lax.div(index, group)
    return section, lax.rem(index, group), (t >= section) & (t < section + batches)


def own_kernel(group, same, t, batches, lens, after, *refs):
    _, me, active = position(group, t, batches)
    n = CHUNKS
    xk = refs[:n]
    refs = refs[n:]
    if same:
        xq = xk
    else:
        xq = refs[:n]
        refs = refs[n:]
    gq, gk, w, acc, sums = refs
    head_cols = w.shape[1] // 3
    share = w.shape[0] // (group * SECTIONS)

    @pl.when(active)
    def _():
        part = me
        lk, sk = scaled(xk, gk, part, group, share, SECTIONS)
        lq, sq = scaled(xq, gq, part, group, share, SECTIONS)

        def emit(start, tile, total):
            acc[:, start : start + tile] = total

        project([lq], [lk], w, [part], group, share, head_cols, emit)
        sums[:, 0:128] = jnp.broadcast_to(sq, (sq.shape[0], 128))
        sums[:, 128:256] = jnp.broadcast_to(sk, (sk.shape[0], 128))


def rest_kernel(group, same, t, batches, lens, after, *refs):
    section, me, active = position(group, t, batches)
    n = CHUNKS * (group - 1)
    xk = refs[:n]
    refs = refs[n:]
    if same:
        xq = xk
    else:
        xq = refs[:n]
        refs = refs[n:]
    gq, gk, w, wo, acc, sums = refs[:6]
    sends = refs[6 : 6 + n]
    mix, qkv = refs[6 + n :]
    head_cols = w.shape[1] // 3
    width = w.shape[0]
    share = width // (group * SECTIONS)
    rows = mix.shape[0]

    @pl.when(active)
    def _():
        parts, lqs, lks = [], [], []
        sq = sums[:, 0:1]
        sk = sums[:, 128:129]
        for k in range(1, group):
            part = lax.rem(me + group - k, group)
            at = CHUNKS * (k - 1)
            lk, s = scaled(xk[at : at + CHUNKS], gk, part, group, share, SECTIONS)
            sk = sk + s
            lq, s = scaled(xq[at : at + CHUNKS], gq, part, group, share, SECTIONS)
            sq = sq + s
            parts.append(part)
            lqs.append(lq)
            lks.append(lk)
        rq = lax.rsqrt(sq / width + epsilon)
        rk = lax.rsqrt(sk / width + epsilon)

        def emit(start, tile, total):
            scale = rq if start < head_cols else rk
            total = (acc[:, start : start + tile] + total) * scale
            qkv[:, start : start + tile] = total.astype(bf16)

        project(lqs, lks, w, parts, group, share, head_cols, emit)

        query = lax.broadcasted_iota(jnp.int32, (rows, rows), 0)
        key = lax.broadcasted_iota(jnp.int32, (rows, rows), 1)
        last = section == SECTIONS - 1
        slot = jnp.clip(t - section, 0, batches - 1) + jnp.where(last, batches, 0)
        allowed = (key < lens[pl.ds(slot, 1), :]) & ((key <= query) | jnp.logical_not(last))
        allowed = jnp.concatenate([allowed.astype(f32)] * 2, 0) > 0.5
        lane = lax.broadcasted_iota(jnp.int32, (rows, 2 * HEAD), 1)
        low = lane < HEAD
        zero = jnp.zeros((), bf16)
        for at in range(0, head_cols, 2 * HEAD):
            q = qkv[:, at : at + 2 * HEAD]
            k = qkv[:, head_cols + at : head_cols + at + 2 * HEAD]
            v = qkv[:, 2 * head_cols + at : 2 * head_cols + at + 2 * HEAD]
            both = jnp.concatenate([jnp.where(low, q, zero), jnp.where(low, zero, q)], 0)
            scores = lax.dot_general(
                both, k, (((1,), (1,)), ((), ())), preferred_element_type=f32
            )
            scores = jnp.where(allowed, scores * score_scale, -1000000000.0)
            top = jnp.max(scores, axis=-1, keepdims=True)
            e = jnp.exp(scores - top)
            weights = (e * (1.0 / jnp.sum(e, axis=-1, keepdims=True))).astype(bf16)
            out = dot(weights, v)
            mix[:, at : at + 2 * HEAD] = jnp.where(low, out[:rows], out[rows:]).astype(bf16)

        mixture = mix[...]
        per = SECTIONS // CHUNKS
        for k in range(1, group):
            part = lax.rem(me + k, group)
            for z in range(SECTIONS):
                ref = sends[(k - 1) * CHUNKS + z // per]
                column = rows_of(z, part, group, share)
                at = (z % per) * share
                ref[:, at : at + share] = dot(mixture, wo[:, column]).astype(bf16)


def tail_kernel(group, t, batches, mix, *refs):
    _, me, active = position(group, t, batches)
    xq = refs[:CHUNKS]
    wo = refs[CHUNKS]
    bases = refs[CHUNKS + 1 :]
    share = wo.shape[1] // (group * SECTIONS)

    @pl.when(active)
    def _():
        mixture = mix[...]
        per = SECTIONS // CHUNKS
        for z in range(SECTIONS):
            column = rows_of(z, me, group, share)
            at = (z % per) * share
            res = xq[z // per][:, at : at + share].astype(f32)
            bases[z // per][:, at : at + share] = dot(mixture, wo[:, column]) + res


def hold_weights(w_in, w_out):
    w_in = pltpu.with_memory_space_constraint(w_in, pltpu.VMEM)
    w_out = pltpu.with_memory_space_constraint(w_out, pltpu.VMEM)

    def touch(a_ref, b_ref, out):
        out[...] = jnp.zeros_like(out)

    token = pl.pallas_call(
        touch,
        out_shape=jax.ShapeDtypeStruct((8, 128), f32),
        in_specs=[VMEM, VMEM],
        out_specs=VMEM,
        compiler_params=params(1 << 20),
        name="touch",
    )(w_in, w_out)
    return w_in, w_out, token


def relay(
    src_embed, tgt_embed, src_lengths, tgt_lengths, attn_in, attn_out, norm_gain, final_gain
):
    axis = "segment"
    segments = lax.axis_size(axis)
    group = segments // SECTIONS
    index = lax.axis_index(axis).astype(jnp.uint32)
    section = lax.div(index, jnp.uint32(group)).astype(jnp.int32)
    member = lax.rem(index, jnp.uint32(group)).astype(jnp.int32)
    at_section = [section == p for p in range(SECTIONS)]
    section, member, at_section = lax.optimization_barrier((section, member, at_section))
    batches, rows, share = src_embed.shape
    part_width = SECTIONS * share
    chunk_width = part_width // CHUNKS
    w_in = attn_in[0]
    w_out = attn_out[0]
    head_cols = w_out.shape[0]
    gain_q = norm_gain[:1]
    for p in range(1, SECTIONS):
        gain_q = jnp.where(at_section[p], norm_gain[p : p + 1], gain_q)
    gain_kv = jnp.where(at_section[2], final_gain[None], gain_q)

    def permute(value, pairs):
        return lax.ppermute(value, axis, pairs)

    def partners(k):
        return [
            (p * group + q, p * group + (q + k) % group)
            for p in range(SECTIONS)
            for q in range(group)
        ]

    def onward(k):
        return [
            (p * group + q, (p + 1) * group + (q + k) % group)
            for p in range(SECTIONS - 1)
            for q in range(group)
        ]

    def shift_pairs(by):
        return [
            (((0 if first else 2) + by) % SECTIONS * group + q, (0 if first else 2) * group + q)
            for first in (True, False)
            for q in range(group)
        ]

    def collect(low, high):
        source = src_embed[low:high]
        target = tgt_embed[low:high]
        payloads = [jnp.where(at_section[by], source, target) for by in range(SECTIONS)]
        payloads = lax.optimization_barrier(payloads)
        pieces = {0: payloads[0]}
        for by in range(1, SECTIONS):
            pieces[by] = permute(payloads[by], shift_pairs(by))
        return pieces

    def part_of(pieces, at):
        rotated = [pieces[by][at] for by in range(SECTIONS)]
        ordered = []
        for z in range(SECTIONS):
            value = rotated[z]
            other = rotated[(z - 2) % SECTIONS]
            ordered.append(jnp.where(at_section[0], value, other))
        width = chunk_width // share
        return [
            jnp.concatenate(ordered[c * width : (c + 1) * width], -1) for c in range(CHUNKS)
        ]

    periods = batches + SECTIONS - 1
    lens = jnp.concatenate([src_lengths, tgt_lengths]).astype(jnp.int32)
    lens = jnp.broadcast_to(lens[:, None], (2 * batches, rows))

    early = collect(0, 1)
    late = [collect(1, batches)]
    w_in, w_out, token = hold_weights(w_in, w_out)
    entry = {}

    def enter(b):
        mine = part_of(early, 0) if b == 0 else part_of(late[0], b - 1)
        mine = lax.optimization_barrier(mine)
        parts = [mine]
        for k in range(1, group):
            parts.append([permute(v, partners(k)) for v in mine])
        entry[b] = parts


    def flat(lists):
        return [v for inner in lists for v in inner]

    def gated(values, gate):
        return lax.optimization_barrier((values, gate))[0]

    def merge(at, ours, theirs):
        return [
            [jnp.where(at_section[at], a, c) for a, c in zip(ra, rc)]
            for ra, rc in zip(ours, theirs)
        ]

    def feed(t, came):
        def select(rows):
            xk = None if came is None else came[rows]
            if t < batches:
                mine = entry[t][rows]
                xk = mine if xk is None else merge(0, mine, xk)
            xq = xk
            if 0 <= t - 2 < batches:
                xq = merge(2, entry[t - 2][rows], xk)
            return xk, xq

        xk, xq = select(slice(0, 1))
        partial = own((t, xk, xq), token)
        if came is not None:
            came = came[:1] + gated(came[1:], partial[1])
        more_k, more_q = select(slice(1, None))
        same = xq is xk
        xk = xk + more_k
        return (t, xk, xk if same else xq + more_q), partial

    def own(fed, after):
        t, xk, xq = fed
        same = xq is xk
        inputs = list(xk[0]) + ([] if same else list(xq[0]))
        return pl.pallas_call(
            functools.partial(own_kernel, group, same, t, batches),
            out_shape=(
                jax.ShapeDtypeStruct((rows, 3 * head_cols), f32),
                jax.ShapeDtypeStruct((rows, 256), f32),
            ),
            in_specs=[VMEM, ANY] + [VMEM] * (len(inputs) + 3),
            out_specs=(VMEM, VMEM),
            compiler_params=params(2 << 20),
            cost_estimate=pl.CostEstimate(
                flops=2 * rows * part_width * 3 * head_cols,
                bytes_accessed=1 << 20,
                transcendentals=0,
            ),
            name="own",
        )(lens, after, *inputs, gain_q, gain_kv, w_in)

    n_send = CHUNKS * (group - 1)

    def rest(fed, partial, after):
        t, xk, xq = fed
        same = xq is xk
        inputs = flat(xk[1:]) + ([] if same else flat(xq[1:]))
        outs = pl.pallas_call(
            functools.partial(rest_kernel, group, same, t, batches),
            out_shape=tuple(
                [jax.ShapeDtypeStruct((rows, chunk_width), bf16)] * n_send
                + [jax.ShapeDtypeStruct((rows, head_cols), bf16)]
            ),
            in_specs=[VMEM, ANY] + [VMEM] * (len(inputs) + 6),
            out_specs=tuple([VMEM] * (n_send + 1)),
            scratch_shapes=[pltpu.VMEM((rows, 3 * head_cols), bf16)],
            compiler_params=params(4 << 20),
            cost_estimate=pl.CostEstimate(
                flops=4 * rows * part_width * 3 * head_cols,
                bytes_accessed=1 << 20,
                transcendentals=rows * rows * (head_cols // HEAD),
            ),
            name="rest",
        )(lens, after, *inputs, gain_q, gain_kv, w_in, w_out, *partial)
        return outs[:n_send], outs[n_send]

    def tail(fed, mix):
        t, _, xq = fed
        return pl.pallas_call(
            functools.partial(tail_kernel, group, t, batches),
            out_shape=tuple([jax.ShapeDtypeStruct((rows, chunk_width), f32)] * CHUNKS),
            in_specs=[VMEM] * (2 + CHUNKS),
            out_specs=tuple([VMEM] * CHUNKS),
            compiler_params=params(1 << 20),
            cost_estimate=pl.CostEstimate(
                flops=2 * rows * part_width * head_cols, bytes_accessed=1 << 20, transcendentals=0
            ),
            name="tail",
        )(mix, *xq[0], w_out)

    enter(0)
    fed, partial = feed(0, None)
    finals = {}
    exits = {}

    def leave(b):
        value = finals[b]
        pieces = []
        for z in range(SECTIONS):
            at, offset = divmod(z * share, chunk_width)
            piece = value[at][:, offset : offset + share]
            if z < SECTIONS - 1:
                pairs = [((SECTIONS - 1) * group + q, z * group + q) for q in range(group)]
                piece = permute(piece, pairs)
            pieces.append(piece)
        result = pieces[-1]
        for z in range(SECTIONS - 1):
            result = jnp.where(at_section[z], pieces[z], result)
        exits[b] = result

    for t in range(periods):
        sends, mix = rest(fed, partial, token)
        bases = tail(fed, mix)
        taken = [
            [permute(sends[(k - 1) * CHUNKS + c], partners(k)) for k in range(1, group)]
            for c in range(CHUNKS)
        ]
        if 0 < t < batches - 1:
            enter(t + 1)
        if t - SECTIONS in finals:
            leave(t - SECTIONS)
        came = [[None] * CHUNKS for _ in range(group)]
        done = []
        for c in range(CHUNKS):
            total = bases[c]
            for v in taken[c]:
                total = total + v.astype(f32)
            total = total.astype(bf16)
            done.append(total)
            if t + 1 < periods:
                for k in range(group):
                    came[k][c] = permute(total, onward(k))
        if t == 0:
            late[0] = gated(late[0], done)
            enter(1)
        if t >= SECTIONS - 1:
            finals[t - SECTIONS + 1] = done
        if t + 1 < periods:
            fed, partial = feed(t + 1, came)
    leave(batches - 1)
    return jnp.stack([exits[b] for b in range(batches)])


def solution(mesh):
    in_specs = (
        P("dp", None, "segment"),
        P("dp", None, "segment"),
        P("dp"),
        P("dp"),
        P("segment", None, None),
        P("segment", None, None),
        P(),
        P(),
    )
    out_specs = P("dp", None, "segment")
    return jax.shard_map(relay, mesh=mesh, in_specs=in_specs, out_specs=out_specs, check_vma=False)
```

```python
import functools

import jax
import jax.numpy as jnp
from jax import lax
from jax.experimental import pallas as pl
from jax.experimental.pallas import tpu as pltpu
from jax.sharding import PartitionSpec as P

HEAD = 64
SECTIONS = 4
CHUNKS = 1

epsilon = 1e-06
score_scale = 0.125


VMEM = pl.BlockSpec(memory_space=pltpu.VMEM)
ANY = pl.BlockSpec(memory_space=pl.ANY)
f32 = jnp.float32
bf16 = jnp.bfloat16


def dot(a, b):
    return jnp.dot(a, b, preferred_element_type=f32)


def column_tile(width):
    return 512 if width % 512 == 0 else width


def params(vmem):
    return pltpu.CompilerParams(vmem_limit_bytes=vmem)


def scaled(x_refs, gain_ref, part, group, share, sections):
    squares = 0.0
    lhs = []
    per = sections // len(x_refs)
    for z in range(sections):
        ref = x_refs[z // per]
        at = (z % per) * share
        x = ref[:, at : at + share].astype(f32)
        squares = squares + jnp.sum(x * x, axis=-1, keepdims=True)
        column = pl.multiple_of((z * group + part) * share, share)
        lhs.append((x * gain_ref[:, pl.ds(column, share)]).astype(bf16))
    return lhs, squares


def rows_of(z, part, group, share):
    return pl.ds(pl.multiple_of((z * group + part) * share, share), share)


def project(lhs_q, lhs_kv, w_ref, parts, group, share, head_cols, emit):
    tile = column_tile(head_cols)
    for start in range(0, 3 * head_cols, tile):
        total = None
        for (part, lq), (_, lk) in zip(zip(parts, lhs_q), zip(parts, lhs_kv)):
            source = lq if start < head_cols else lk
            for z, block in enumerate(source):
                rows = rows_of(z, part, group, share)
                term = dot(block, w_ref[rows, start : start + tile])
                total = term if total is None else total + term
        emit(start, tile, total)


def position(group, t, batches):
    index = lax.axis_index("segment")
    section = lax.div(index, group)
    return section, lax.rem(index, group), (t >= section) & (t < section + batches)


def own_kernel(group, same, t, batches, lens, after, *refs):
    _, me, active = position(group, t, batches)
    n = CHUNKS
    xk = refs[:n]
    refs = refs[n:]
    if same:
        xq = xk
    else:
        xq = refs[:n]
        refs = refs[n:]
    gq, gk, w, acc, sums = refs
    head_cols = w.shape[1] // 3
    share = w.shape[0] // (group * SECTIONS)

    @pl.when(active)
    def _():
        part = me
        lk, sk = scaled(xk, gk, part, group, share, SECTIONS)
        lq, sq = scaled(xq, gq, part, group, share, SECTIONS)

        def emit(start, tile, total):
            acc[:, start : start + tile] = total

        project([lq], [lk], w, [part], group, share, head_cols, emit)
        sums[:, 0:128] = jnp.broadcast_to(sq, (sq.shape[0], 128))
        sums[:, 128:256] = jnp.broadcast_to(sk, (sk.shape[0], 128))


def rest_kernel(group, same, t, batches, lens, after, *refs):
    section, me, active = position(group, t, batches)
    n = CHUNKS * (group - 1)
    xk = refs[:n]
    refs = refs[n:]
    if same:
        xq = xk
    else:
        xq = refs[:n]
        refs = refs[n:]
    gq, gk, w, wo, acc, sums = refs[:6]
    sends = refs[6 : 6 + n]
    mix, qkv = refs[6 + n :]
    head_cols = w.shape[1] // 3
    width = w.shape[0]
    share = width // (group * SECTIONS)
    rows = mix.shape[0]

    @pl.when(active)
    def _():
        parts, lqs, lks = [], [], []
        sq = sums[:, 0:1]
        sk = sums[:, 128:129]
        for k in range(1, group):
            part = lax.rem(me + group - k, group)
            at = CHUNKS * (k - 1)
            lk, s = scaled(xk[at : at + CHUNKS], gk, part, group, share, SECTIONS)
            sk = sk + s
            lq, s = scaled(xq[at : at + CHUNKS], gq, part, group, share, SECTIONS)
            sq = sq + s
            parts.append(part)
            lqs.append(lq)
            lks.append(lk)
        rq = lax.rsqrt(sq / width + epsilon)
        rk = lax.rsqrt(sk / width + epsilon)

        def emit(start, tile, total):
            scale = rq if start < head_cols else rk
            total = (acc[:, start : start + tile] + total) * scale
            qkv[:, start : start + tile] = total.astype(bf16)

        project(lqs, lks, w, parts, group, share, head_cols, emit)

        query = lax.broadcasted_iota(jnp.int32, (rows, rows), 0)
        key = lax.broadcasted_iota(jnp.int32, (rows, rows), 1)
        last = section == SECTIONS - 1
        slot = jnp.clip(t - section, 0, batches - 1) + jnp.where(last, batches, 0)
        allowed = (key < lens[pl.ds(slot, 1), :]) & ((key <= query) | jnp.logical_not(last))
        allowed = jnp.concatenate([allowed.astype(f32)] * 2, 0) > 0.5
        lane = lax.broadcasted_iota(jnp.int32, (rows, 2 * HEAD), 1)
        low = lane < HEAD
        zero = jnp.zeros((), bf16)
        for at in range(0, head_cols, 2 * HEAD):
            q = qkv[:, at : at + 2 * HEAD]
            k = qkv[:, head_cols + at : head_cols + at + 2 * HEAD]
            v = qkv[:, 2 * head_cols + at : 2 * head_cols + at + 2 * HEAD]
            both = jnp.concatenate([jnp.where(low, q, zero), jnp.where(low, zero, q)], 0)
            scores = lax.dot_general(
                both, k, (((1,), (1,)), ((), ())), preferred_element_type=f32
            )
            scores = jnp.where(allowed, scores * score_scale, -1000000000.0)
            top = jnp.max(scores, axis=-1, keepdims=True)
            e = jnp.exp(scores - top)
            weights = (e * (1.0 / jnp.sum(e, axis=-1, keepdims=True))).astype(bf16)
            out = dot(weights, v)
            mix[:, at : at + 2 * HEAD] = jnp.where(low, out[:rows], out[rows:]).astype(bf16)

        mixture = mix[...]
        per = SECTIONS // CHUNKS
        for k in range(1, group):
            part = lax.rem(me + k, group)
            for z in range(SECTIONS):
                ref = sends[(k - 1) * CHUNKS + z // per]
                column = rows_of(z, part, group, share)
                at = (z % per) * share
                ref[:, at : at + share] = dot(mixture, wo[:, column]).astype(bf16)


def tail_kernel(group, t, batches, mix, *refs):
    _, me, active = position(group, t, batches)
    xq = refs[:CHUNKS]
    wo = refs[CHUNKS]
    bases = refs[CHUNKS + 1 :]
    share = wo.shape[1] // (group * SECTIONS)

    @pl.when(active)
    def _():
        mixture = mix[...]
        per = SECTIONS // CHUNKS
        for z in range(SECTIONS):
            column = rows_of(z, me, group, share)
            at = (z % per) * share
            res = xq[z // per][:, at : at + share].astype(f32)
            bases[z // per][:, at : at + share] = dot(mixture, wo[:, column]) + res


def hold_weights(w_in, w_out):
    w_in = pltpu.with_memory_space_constraint(w_in, pltpu.VMEM)
    w_out = pltpu.with_memory_space_constraint(w_out, pltpu.VMEM)

    def touch(a_ref, b_ref, out):
        out[...] = jnp.zeros_like(out)

    token = pl.pallas_call(
        touch,
        out_shape=jax.ShapeDtypeStruct((8, 128), f32),
        in_specs=[VMEM, VMEM],
        out_specs=VMEM,
        compiler_params=params(1 << 20),
        name="touch",
    )(w_in, w_out)
    return w_in, w_out, token


def relay(
    src_embed, tgt_embed, src_lengths, tgt_lengths, attn_in, attn_out, norm_gain, final_gain
):
    axis = "segment"
    segments = lax.axis_size(axis)
    group = segments // SECTIONS
    index = lax.axis_index(axis).astype(jnp.uint32)
    section = lax.div(index, jnp.uint32(group)).astype(jnp.int32)
    member = lax.rem(index, jnp.uint32(group)).astype(jnp.int32)
    at_section = [section == p for p in range(SECTIONS)]
    section, member, at_section = lax.optimization_barrier((section, member, at_section))
    batches, rows, share = src_embed.shape
    part_width = SECTIONS * share
    chunk_width = part_width // CHUNKS
    w_in = attn_in[0]
    w_out = attn_out[0]
    head_cols = w_out.shape[0]
    gain_q = norm_gain[:1]
    for p in range(1, SECTIONS):
        gain_q = jnp.where(at_section[p], norm_gain[p : p + 1], gain_q)
    gain_kv = jnp.where(at_section[2], final_gain[None], gain_q)

    def permute(value, pairs):
        return lax.ppermute(value, axis, pairs)

    def partners(k):
        return [
            (p * group + q, p * group + (q + k) % group)
            for p in range(SECTIONS)
            for q in range(group)
        ]

    def onward(k):
        return [
            (p * group + q, (p + 1) * group + (q + k) % group)
            for p in range(SECTIONS - 1)
            for q in range(group)
        ]

    def shift_pairs(by):
        return [
            (((0 if first else 2) + by) % SECTIONS * group + q, (0 if first else 2) * group + q)
            for first in (True, False)
            for q in range(group)
        ]

    def collect(low, high):
        source = src_embed[low:high]
        target = tgt_embed[low:high]
        payloads = [jnp.where(at_section[by], source, target) for by in range(SECTIONS)]
        payloads = lax.optimization_barrier(payloads)
        pieces = {0: payloads[0]}
        for by in range(1, SECTIONS):
            pieces[by] = permute(payloads[by], shift_pairs(by))
        return pieces

    def part_of(pieces, at):
        rotated = [pieces[by][at] for by in range(SECTIONS)]
        ordered = []
        for z in range(SECTIONS):
            value = rotated[z]
            other = rotated[(z - 2) % SECTIONS]
            ordered.append(jnp.where(at_section[0], value, other))
        width = chunk_width // share
        return [
            jnp.concatenate(ordered[c * width : (c + 1) * width], -1) for c in range(CHUNKS)
        ]

    periods = batches + SECTIONS - 1
    lens = jnp.concatenate([src_lengths, tgt_lengths]).astype(jnp.int32)
    lens = jnp.broadcast_to(lens[:, None], (2 * batches, rows))

    early = collect(0, 1)
    late = [collect(1, batches)]
    w_in, w_out, token = hold_weights(w_in, w_out)
    entry = {}

    def enter(b):
        mine = part_of(early, 0) if b == 0 else part_of(late[0], b - 1)
        mine = lax.optimization_barrier(mine)
        parts = [mine]
        for k in range(1, group):
            parts.append([permute(v, partners(k)) for v in mine])
        entry[b] = parts


    def flat(lists):
        return [v for inner in lists for v in inner]

    def gated(values, gate):
        return lax.optimization_barrier((values, gate))[0]

    def merge(at, ours, theirs):
        return [
            [jnp.where(at_section[at], a, c) for a, c in zip(ra, rc)]
            for ra, rc in zip(ours, theirs)
        ]

    def feed(t, came):
        def select(rows):
            xk = None if came is None else came[rows]
            if t < batches:
                mine = entry[t][rows]
                xk = mine if xk is None else merge(0, mine, xk)
            xq = xk
            if 0 <= t - 2 < batches:
                xq = merge(2, entry[t - 2][rows], xk)
            return xk, xq

        xk, xq = select(slice(0, 1))
        partial = own((t, xk, xq), token)
        if came is not None:
            came = came[:1] + gated(came[1:], partial[1])
        more_k, more_q = select(slice(1, None))
        same = xq is xk
        xk = xk + more_k
        return (t, xk, xk if same else xq + more_q), partial

    def own(fed, after):
        t, xk, xq = fed
        same = xq is xk
        inputs = list(xk[0]) + ([] if same else list(xq[0]))
        return pl.pallas_call(
            functools.partial(own_kernel, group, same, t, batches),
            out_shape=(
                jax.ShapeDtypeStruct((rows, 3 * head_cols), f32),
                jax.ShapeDtypeStruct((rows, 256), f32),
            ),
            in_specs=[VMEM, ANY] + [VMEM] * (len(inputs) + 3),
            out_specs=(VMEM, VMEM),
            compiler_params=params(2 << 20),
            cost_estimate=pl.CostEstimate(
                flops=2 * rows * part_width * 3 * head_cols,
                bytes_accessed=1 << 20,
                transcendentals=0,
            ),
            name="own",
        )(lens, after, *inputs, gain_q, gain_kv, w_in)

    n_send = CHUNKS * (group - 1)

    def rest(fed, partial, after):
        t, xk, xq = fed
        same = xq is xk
        inputs = flat(xk[1:]) + ([] if same else flat(xq[1:]))
        outs = pl.pallas_call(
            functools.partial(rest_kernel, group, same, t, batches),
            out_shape=tuple(
                [jax.ShapeDtypeStruct((rows, chunk_width), bf16)] * n_send
                + [jax.ShapeDtypeStruct((rows, head_cols), bf16)]
            ),
            in_specs=[VMEM, ANY] + [VMEM] * (len(inputs) + 6),
            out_specs=tuple([VMEM] * (n_send + 1)),
            scratch_shapes=[pltpu.VMEM((rows, 3 * head_cols), bf16)],
            compiler_params=params(4 << 20),
            cost_estimate=pl.CostEstimate(
                flops=4 * rows * part_width * 3 * head_cols,
                bytes_accessed=1 << 20,
                transcendentals=rows * rows * (head_cols // HEAD),
            ),
            name="rest",
        )(lens, after, *inputs, gain_q, gain_kv, w_in, w_out, *partial)
        return outs[:n_send], outs[n_send]

    def tail(fed, mix):
        t, _, xq = fed
        return pl.pallas_call(
            functools.partial(tail_kernel, group, t, batches),
            out_shape=tuple([jax.ShapeDtypeStruct((rows, chunk_width), f32)] * CHUNKS),
            in_specs=[VMEM] * (2 + CHUNKS),
            out_specs=tuple([VMEM] * CHUNKS),
            compiler_params=params(1 << 20),
            cost_estimate=pl.CostEstimate(
                flops=2 * rows * part_width * head_cols, bytes_accessed=1 << 20, transcendentals=0
            ),
            name="tail",
        )(mix, *xq[0], w_out)

    enter(0)
    fed, partial = feed(0, None)
    finals = {}
    exits = []

    def leave(slots):
        pieces = []
        for z in range(SECTIONS):
            at, offset = divmod(z * share, chunk_width)
            piece = jnp.stack([finals[b][at][:, offset : offset + share] for b in slots])
            if z < SECTIONS - 1:
                pairs = [((SECTIONS - 1) * group + q, z * group + q) for q in range(group)]
                piece = permute(piece, pairs)
            pieces.append(piece)
        result = pieces[-1]
        for z in range(SECTIONS - 1):
            result = jnp.where(at_section[z], pieces[z], result)
        exits.append(result)

    for t in range(periods):
        sends, mix = rest(fed, partial, token)
        bases = tail(fed, mix)
        taken = [
            [permute(sends[(k - 1) * CHUNKS + c], partners(k)) for k in range(1, group)]
            for c in range(CHUNKS)
        ]
        if 0 < t < batches - 1:
            enter(t + 1)
        if t + 1 == periods and batches > 1:
            leave(range(batches - 1))
        came = [[None] * CHUNKS for _ in range(group)]
        done = []
        for c in range(CHUNKS):
            total = bases[c]
            for v in taken[c]:
                total = total + v.astype(f32)
            total = total.astype(bf16)
            done.append(total)
            if t + 1 < periods:
                for k in range(group):
                    came[k][c] = permute(total, onward(k))
        if t == 0:
            late[0] = gated(late[0], done)
            enter(1)
        if t >= SECTIONS - 1:
            finals[t - SECTIONS + 1] = done
        if t + 1 < periods:
            fed, partial = feed(t + 1, came)
    leave(range(batches - 1, batches))
    return jnp.concatenate(exits)


def solution(mesh):
    in_specs = (
        P("dp", None, "segment"),
        P("dp", None, "segment"),
        P("dp"),
        P("dp"),
        P("segment", None, None),
        P("segment", None, None),
        P(),
        P(),
    )
    out_specs = P("dp", None, "segment")
    return jax.shard_map(relay, mesh=mesh, in_specs=in_specs, out_specs=out_specs, check_vma=False)
```

```python
import functools

import jax
import jax.numpy as jnp
from jax import lax
from jax.experimental import pallas as pl
from jax.experimental.pallas import tpu as pltpu
from jax.sharding import PartitionSpec as P

HEAD = 64
SECTIONS = 4
CHUNKS = 1

epsilon = 1e-06
score_scale = 0.125


VMEM = pl.BlockSpec(memory_space=pltpu.VMEM)
ANY = pl.BlockSpec(memory_space=pl.ANY)
f32 = jnp.float32
bf16 = jnp.bfloat16


def dot(a, b):
    return jnp.dot(a, b, preferred_element_type=f32)


def column_tile(width):
    return 512 if width % 512 == 0 else width


def params(vmem):
    return pltpu.CompilerParams(vmem_limit_bytes=vmem)


def scaled(x_refs, gain_ref, part, group, share, sections):
    squares = 0.0
    lhs = []
    per = sections // len(x_refs)
    for z in range(sections):
        ref = x_refs[z // per]
        at = (z % per) * share
        x = ref[:, at : at + share].astype(f32)
        squares = squares + jnp.sum(x * x, axis=-1, keepdims=True)
        column = pl.multiple_of((z * group + part) * share, share)
        lhs.append((x * gain_ref[:, pl.ds(column, share)]).astype(bf16))
    return lhs, squares


def rows_of(z, part, group, share):
    return pl.ds(pl.multiple_of((z * group + part) * share, share), share)


def project(lhs_q, lhs_kv, w_ref, parts, group, share, head_cols, emit):
    tile = column_tile(head_cols)
    for start in range(0, 3 * head_cols, tile):
        total = None
        for (part, lq), (_, lk) in zip(zip(parts, lhs_q), zip(parts, lhs_kv)):
            source = lq if start < head_cols else lk
            for z, block in enumerate(source):
                rows = rows_of(z, part, group, share)
                term = dot(block, w_ref[rows, start : start + tile])
                total = term if total is None else total + term
        emit(start, tile, total)


def position(group, t, batches):
    index = lax.axis_index("segment")
    section = lax.div(index, group)
    return section, lax.rem(index, group), (t >= section) & (t < section + batches)


def own_kernel(group, same, t, batches, lens, after, *refs):
    _, me, active = position(group, t, batches)
    n = CHUNKS
    xk = refs[:n]
    refs = refs[n:]
    if same:
        xq = xk
    else:
        xq = refs[:n]
        refs = refs[n:]
    gq, gk, w, acc, sums = refs
    head_cols = w.shape[1] // 3
    share = w.shape[0] // (group * SECTIONS)

    @pl.when(active)
    def _():
        part = me
        lk, sk = scaled(xk, gk, part, group, share, SECTIONS)
        lq, sq = scaled(xq, gq, part, group, share, SECTIONS)

        def emit(start, tile, total):
            acc[:, start : start + tile] = total

        project([lq], [lk], w, [part], group, share, head_cols, emit)
        sums[:, 0:128] = jnp.broadcast_to(sq, (sq.shape[0], 128))
        sums[:, 128:256] = jnp.broadcast_to(sk, (sk.shape[0], 128))


def rest_kernel(group, same, t, batches, lens, after, *refs):
    section, me, active = position(group, t, batches)
    n = CHUNKS * (group - 1)
    xk = refs[:n]
    refs = refs[n:]
    if same:
        xq = xk
    else:
        xq = refs[:n]
        refs = refs[n:]
    gq, gk, w, wo, acc, sums = refs[:6]
    sends = refs[6 : 6 + n]
    mix, qkv = refs[6 + n :]
    head_cols = w.shape[1] // 3
    width = w.shape[0]
    share = width // (group * SECTIONS)
    rows = mix.shape[0]

    @pl.when(active)
    def _():
        parts, lqs, lks = [], [], []
        sq = sums[:, 0:1]
        sk = sums[:, 128:129]
        for k in range(1, group):
            part = lax.rem(me + group - k, group)
            at = CHUNKS * (k - 1)
            lk, s = scaled(xk[at : at + CHUNKS], gk, part, group, share, SECTIONS)
            sk = sk + s
            lq, s = scaled(xq[at : at + CHUNKS], gq, part, group, share, SECTIONS)
            sq = sq + s
            parts.append(part)
            lqs.append(lq)
            lks.append(lk)
        rq = lax.rsqrt(sq / width + epsilon)
        rk = lax.rsqrt(sk / width + epsilon)

        def emit(start, tile, total):
            scale = rq if start < head_cols else rk
            total = (acc[:, start : start + tile] + total) * scale
            qkv[:, start : start + tile] = total.astype(bf16)

        project(lqs, lks, w, parts, group, share, head_cols, emit)

        query = lax.broadcasted_iota(jnp.int32, (rows, rows), 0)
        key = lax.broadcasted_iota(jnp.int32, (rows, rows), 1)
        last = section == SECTIONS - 1
        slot = jnp.clip(t - section, 0, batches - 1) + jnp.where(last, batches, 0)
        allowed = (key < lens[pl.ds(slot, 1), :]) & ((key <= query) | jnp.logical_not(last))
        allowed = jnp.concatenate([allowed.astype(f32)] * 2, 0) > 0.5
        lane = lax.broadcasted_iota(jnp.int32, (rows, 2 * HEAD), 1)
        low = lane < HEAD
        zero = jnp.zeros((), bf16)
        for at in range(0, head_cols, 2 * HEAD):
            q = qkv[:, at : at + 2 * HEAD]
            k = qkv[:, head_cols + at : head_cols + at + 2 * HEAD]
            v = qkv[:, 2 * head_cols + at : 2 * head_cols + at + 2 * HEAD]
            both = jnp.concatenate([jnp.where(low, q, zero), jnp.where(low, zero, q)], 0)
            scores = lax.dot_general(
                both, k, (((1,), (1,)), ((), ())), preferred_element_type=f32
            )
            scores = jnp.where(allowed, scores * score_scale, -1000000000.0)
            top = jnp.max(scores, axis=-1, keepdims=True)
            e = jnp.exp(scores - top)
            weights = (e * (1.0 / jnp.sum(e, axis=-1, keepdims=True))).astype(bf16)
            out = dot(weights, v)
            mix[:, at : at + 2 * HEAD] = jnp.where(low, out[:rows], out[rows:]).astype(bf16)

        mixture = mix[...]
        per = SECTIONS // CHUNKS
        for k in range(1, group):
            part = lax.rem(me + k, group)
            for z in range(SECTIONS):
                ref = sends[(k - 1) * CHUNKS + z // per]
                column = rows_of(z, part, group, share)
                at = (z % per) * share
                ref[:, at : at + share] = dot(mixture, wo[:, column]).astype(bf16)


def tail_kernel(group, t, batches, mix, *refs):
    _, me, active = position(group, t, batches)
    xq = refs[:CHUNKS]
    wo = refs[CHUNKS]
    bases = refs[CHUNKS + 1 :]
    share = wo.shape[1] // (group * SECTIONS)

    @pl.when(active)
    def _():
        mixture = mix[...]
        per = SECTIONS // CHUNKS
        for z in range(SECTIONS):
            column = rows_of(z, me, group, share)
            at = (z % per) * share
            res = xq[z // per][:, at : at + share].astype(f32)
            bases[z // per][:, at : at + share] = dot(mixture, wo[:, column]) + res


def hold_weights(w_in, w_out):
    w_in = pltpu.with_memory_space_constraint(w_in, pltpu.VMEM)
    w_out = pltpu.with_memory_space_constraint(w_out, pltpu.VMEM)

    def touch(a_ref, out):
        out[...] = jnp.zeros_like(out)

    token = pl.pallas_call(
        touch,
        out_shape=jax.ShapeDtypeStruct((8, 128), f32),
        in_specs=[VMEM],
        out_specs=VMEM,
        compiler_params=params(1 << 20),
        name="touch",
    )(w_in)
    return w_in, w_out, token


def relay(
    src_embed, tgt_embed, src_lengths, tgt_lengths, attn_in, attn_out, norm_gain, final_gain
):
    axis = "segment"
    segments = lax.axis_size(axis)
    group = segments // SECTIONS
    index = lax.axis_index(axis).astype(jnp.uint32)
    section = lax.div(index, jnp.uint32(group)).astype(jnp.int32)
    member = lax.rem(index, jnp.uint32(group)).astype(jnp.int32)
    at_section = [section == p for p in range(SECTIONS)]
    section, member, at_section = lax.optimization_barrier((section, member, at_section))
    batches, rows, share = src_embed.shape
    part_width = SECTIONS * share
    chunk_width = part_width // CHUNKS
    w_in = attn_in[0]
    w_out = attn_out[0]
    head_cols = w_out.shape[0]
    gain_q = norm_gain[:1]
    for p in range(1, SECTIONS):
        gain_q = jnp.where(at_section[p], norm_gain[p : p + 1], gain_q)
    gain_kv = jnp.where(at_section[2], final_gain[None], gain_q)

    def permute(value, pairs):
        return lax.ppermute(value, axis, pairs)

    def partners(k):
        return [
            (p * group + q, p * group + (q + k) % group)
            for p in range(SECTIONS)
            for q in range(group)
        ]

    def onward(k):
        return [
            (p * group + q, (p + 1) * group + (q + k) % group)
            for p in range(SECTIONS - 1)
            for q in range(group)
        ]

    def shift_pairs(by):
        return [
            (((0 if first else 2) + by) % SECTIONS * group + q, (0 if first else 2) * group + q)
            for first in (True, False)
            for q in range(group)
        ]

    def collect(low, high):
        source = src_embed[low:high]
        target = tgt_embed[low:high]
        payloads = [jnp.where(at_section[by], source, target) for by in range(SECTIONS)]
        payloads = lax.optimization_barrier(payloads)
        pieces = {0: payloads[0]}
        for by in range(1, SECTIONS):
            pieces[by] = permute(payloads[by], shift_pairs(by))
        return pieces

    def part_of(pieces, at):
        rotated = [pieces[by][at] for by in range(SECTIONS)]
        ordered = []
        for z in range(SECTIONS):
            value = rotated[z]
            other = rotated[(z - 2) % SECTIONS]
            ordered.append(jnp.where(at_section[0], value, other))
        width = chunk_width // share
        return [
            jnp.concatenate(ordered[c * width : (c + 1) * width], -1) for c in range(CHUNKS)
        ]

    periods = batches + SECTIONS - 1
    lens = jnp.concatenate([src_lengths, tgt_lengths]).astype(jnp.int32)
    lens = jnp.broadcast_to(lens[:, None], (2 * batches, rows))

    early = collect(0, 1)
    late = [collect(1, batches)]
    w_in, w_out, token = hold_weights(w_in, w_out)
    entry = {}

    def enter(b):
        mine = part_of(early, 0) if b == 0 else part_of(late[0], b - 1)
        mine = lax.optimization_barrier(mine)
        parts = [mine]
        for k in range(1, group):
            parts.append([permute(v, partners(k)) for v in mine])
        entry[b] = parts


    def flat(lists):
        return [v for inner in lists for v in inner]

    def gated(values, gate):
        return lax.optimization_barrier((values, gate))[0]

    def merge(at, ours, theirs):
        return [
            [jnp.where(at_section[at], a, c) for a, c in zip(ra, rc)]
            for ra, rc in zip(ours, theirs)
        ]

    def feed(t, came):
        def select(rows):
            xk = None if came is None else came[rows]
            if t < batches:
                mine = entry[t][rows]
                xk = mine if xk is None else merge(0, mine, xk)
            xq = xk
            if 0 <= t - 2 < batches:
                xq = merge(2, entry[t - 2][rows], xk)
            return xk, xq

        xk, xq = select(slice(0, 1))
        partial = own((t, xk, xq), token)
        if came is not None:
            came = came[:1] + gated(came[1:], partial[1])
        more_k, more_q = select(slice(1, None))
        same = xq is xk
        xk = xk + more_k
        return (t, xk, xk if same else xq + more_q), partial

    def own(fed, after):
        t, xk, xq = fed
        same = xq is xk
        inputs = list(xk[0]) + ([] if same else list(xq[0]))
        return pl.pallas_call(
            functools.partial(own_kernel, group, same, t, batches),
            out_shape=(
                jax.ShapeDtypeStruct((rows, 3 * head_cols), f32),
                jax.ShapeDtypeStruct((rows, 256), f32),
            ),
            in_specs=[VMEM, ANY] + [VMEM] * (len(inputs) + 3),
            out_specs=(VMEM, VMEM),
            compiler_params=params(2 << 20),
            cost_estimate=pl.CostEstimate(
                flops=2 * rows * part_width * 3 * head_cols,
                bytes_accessed=1 << 20,
                transcendentals=0,
            ),
            name="own",
        )(lens, after, *inputs, gain_q, gain_kv, w_in)

    n_send = CHUNKS * (group - 1)

    def rest(fed, partial, after):
        t, xk, xq = fed
        same = xq is xk
        inputs = flat(xk[1:]) + ([] if same else flat(xq[1:]))
        outs = pl.pallas_call(
            functools.partial(rest_kernel, group, same, t, batches),
            out_shape=tuple(
                [jax.ShapeDtypeStruct((rows, chunk_width), bf16)] * n_send
                + [jax.ShapeDtypeStruct((rows, head_cols), bf16)]
            ),
            in_specs=[VMEM, ANY] + [VMEM] * (len(inputs) + 6),
            out_specs=tuple([VMEM] * (n_send + 1)),
            scratch_shapes=[pltpu.VMEM((rows, 3 * head_cols), bf16)],
            compiler_params=params(4 << 20),
            cost_estimate=pl.CostEstimate(
                flops=4 * rows * part_width * 3 * head_cols,
                bytes_accessed=1 << 20,
                transcendentals=rows * rows * (head_cols // HEAD),
            ),
            name="rest",
        )(lens, after, *inputs, gain_q, gain_kv, w_in, w_out, *partial)
        return outs[:n_send], outs[n_send]

    def tail(fed, mix):
        t, _, xq = fed
        return pl.pallas_call(
            functools.partial(tail_kernel, group, t, batches),
            out_shape=tuple([jax.ShapeDtypeStruct((rows, chunk_width), f32)] * CHUNKS),
            in_specs=[VMEM] * (2 + CHUNKS),
            out_specs=tuple([VMEM] * CHUNKS),
            compiler_params=params(1 << 20),
            cost_estimate=pl.CostEstimate(
                flops=2 * rows * part_width * head_cols, bytes_accessed=1 << 20, transcendentals=0
            ),
            name="tail",
        )(mix, *xq[0], w_out)

    enter(0)
    fed, partial = feed(0, None)
    finals = {}
    exits = []

    def leave(slots):
        pieces = []
        for z in range(SECTIONS):
            at, offset = divmod(z * share, chunk_width)
            piece = jnp.stack([finals[b][at][:, offset : offset + share] for b in slots])
            if z < SECTIONS - 1:
                pairs = [((SECTIONS - 1) * group + q, z * group + q) for q in range(group)]
                piece = permute(piece, pairs)
            pieces.append(piece)
        result = pieces[-1]
        for z in range(SECTIONS - 1):
            result = jnp.where(at_section[z], pieces[z], result)
        exits.append(result)

    for t in range(periods):
        sends, mix = rest(fed, partial, token)
        bases = tail(fed, mix)
        taken = [
            [permute(sends[(k - 1) * CHUNKS + c], partners(k)) for k in range(1, group)]
            for c in range(CHUNKS)
        ]
        if 0 < t < batches - 1:
            enter(t + 1)
        if t + 1 == periods and batches > 1:
            leave(range(batches - 1))
        came = [[None] * CHUNKS for _ in range(group)]
        done = []
        for c in range(CHUNKS):
            total = bases[c]
            for v in taken[c]:
                total = total + v.astype(f32)
            total = total.astype(bf16)
            done.append(total)
            if t + 1 < periods:
                for k in range(group):
                    came[k][c] = permute(total, onward(k))
        if t == 0:
            late[0] = gated(late[0], done)
            enter(1)
        if t >= SECTIONS - 1:
            finals[t - SECTIONS + 1] = done
        if t + 1 < periods:
            fed, partial = feed(t + 1, came)
    leave(range(batches - 1, batches))
    return jnp.concatenate(exits)


def solution(mesh):
    in_specs = (
        P("dp", None, "segment"),
        P("dp", None, "segment"),
        P("dp"),
        P("dp"),
        P("segment", None, None),
        P("segment", None, None),
        P(),
        P(),
    )
    out_specs = P("dp", None, "segment")
    return jax.shard_map(relay, mesh=mesh, in_specs=in_specs, out_specs=out_specs, check_vma=False)
```

```python
import functools

import jax
import jax.numpy as jnp
from jax import lax
from jax.experimental import pallas as pl
from jax.experimental.pallas import tpu as pltpu
from jax.sharding import PartitionSpec as P

HEAD = 64
SECTIONS = 4
CHUNKS = 1

epsilon = 1e-06
score_scale = 0.125


VMEM = pl.BlockSpec(memory_space=pltpu.VMEM)
ANY = pl.BlockSpec(memory_space=pl.ANY)
f32 = jnp.float32
bf16 = jnp.bfloat16


def dot(a, b):
    return jnp.dot(a, b, preferred_element_type=f32)


def column_tile(width):
    return 512 if width % 512 == 0 else width


def params(vmem):
    return pltpu.CompilerParams(vmem_limit_bytes=vmem)


def scaled(x_refs, gain_ref, part, group, share, sections):
    squares = 0.0
    lhs = []
    per = sections // len(x_refs)
    for z in range(sections):
        ref = x_refs[z // per]
        at = (z % per) * share
        x = ref[:, at : at + share].astype(f32)
        squares = squares + jnp.sum(x * x, axis=-1, keepdims=True)
        column = pl.multiple_of((z * group + part) * share, share)
        lhs.append((x * gain_ref[:, pl.ds(column, share)]).astype(bf16))
    return lhs, squares


def rows_of(z, part, group, share):
    return pl.ds(pl.multiple_of((z * group + part) * share, share), share)


def project(lhs_q, lhs_kv, w_ref, parts, group, share, head_cols, emit):
    tile = column_tile(head_cols)
    for start in range(0, 3 * head_cols, tile):
        total = None
        for (part, lq), (_, lk) in zip(zip(parts, lhs_q), zip(parts, lhs_kv)):
            source = lq if start < head_cols else lk
            for z, block in enumerate(source):
                rows = rows_of(z, part, group, share)
                term = dot(block, w_ref[rows, start : start + tile])
                total = term if total is None else total + term
        emit(start, tile, total)


def position(group, t, batches):
    index = lax.axis_index("segment")
    section = lax.div(index, group)
    return section, lax.rem(index, group), (t >= section) & (t < section + batches)


def own_kernel(group, same, t, batches, lens, after, *refs):
    _, me, active = position(group, t, batches)
    n = CHUNKS
    xk = refs[:n]
    refs = refs[n:]
    if same:
        xq = xk
    else:
        xq = refs[:n]
        refs = refs[n:]
    gq, gk, w, acc, sums = refs
    head_cols = w.shape[1] // 3
    share = w.shape[0] // (group * SECTIONS)

    @pl.when(active)
    def _():
        part = me
        lk, sk = scaled(xk, gk, part, group, share, SECTIONS)
        lq, sq = scaled(xq, gq, part, group, share, SECTIONS)

        def emit(start, tile, total):
            acc[:, start : start + tile] = total

        project([lq], [lk], w, [part], group, share, head_cols, emit)
        sums[:, 0:128] = jnp.broadcast_to(sq, (sq.shape[0], 128))
        sums[:, 128:256] = jnp.broadcast_to(sk, (sk.shape[0], 128))


def rest_kernel(group, same, t, batches, lens, after, *refs):
    section, me, active = position(group, t, batches)
    n = CHUNKS * (group - 1)
    xk = refs[:n]
    refs = refs[n:]
    if same:
        xq = xk
    else:
        xq = refs[:n]
        refs = refs[n:]
    gq, gk, w, wo, acc, sums = refs[:6]
    sends = refs[6 : 6 + n]
    mix, qkv = refs[6 + n :]
    head_cols = w.shape[1] // 3
    width = w.shape[0]
    share = width // (group * SECTIONS)
    rows = mix.shape[0]

    @pl.when(active)
    def _():
        parts, lqs, lks = [], [], []
        sq = sums[:, 0:1]
        sk = sums[:, 128:129]
        for k in range(1, group):
            part = lax.rem(me + group - k, group)
            at = CHUNKS * (k - 1)
            lk, s = scaled(xk[at : at + CHUNKS], gk, part, group, share, SECTIONS)
            sk = sk + s
            lq, s = scaled(xq[at : at + CHUNKS], gq, part, group, share, SECTIONS)
            sq = sq + s
            parts.append(part)
            lqs.append(lq)
            lks.append(lk)
        rq = lax.rsqrt(sq / width + epsilon)
        rk = lax.rsqrt(sk / width + epsilon)

        def emit(start, tile, total):
            scale = rq if start < head_cols else rk
            total = (acc[:, start : start + tile] + total) * scale
            qkv[:, start : start + tile] = total.astype(bf16)

        project(lqs, lks, w, parts, group, share, head_cols, emit)

        query = lax.broadcasted_iota(jnp.int32, (rows, rows), 0)
        key = lax.broadcasted_iota(jnp.int32, (rows, rows), 1)
        last = section == SECTIONS - 1
        slot = jnp.clip(t - section, 0, batches - 1) + jnp.where(last, batches, 0)
        allowed = (key < lens[pl.ds(slot, 1), :]) & ((key <= query) | jnp.logical_not(last))
        allowed = jnp.concatenate([allowed.astype(f32)] * 2, 0) > 0.5
        lane = lax.broadcasted_iota(jnp.int32, (rows, 2 * HEAD), 1)
        low = lane < HEAD
        zero = jnp.zeros((), bf16)
        for at in range(0, head_cols, 2 * HEAD):
            q = qkv[:, at : at + 2 * HEAD]
            k = qkv[:, head_cols + at : head_cols + at + 2 * HEAD]
            v = qkv[:, 2 * head_cols + at : 2 * head_cols + at + 2 * HEAD]
            both = jnp.concatenate([jnp.where(low, q, zero), jnp.where(low, zero, q)], 0)
            scores = lax.dot_general(
                both, k, (((1,), (1,)), ((), ())), preferred_element_type=f32
            )
            scores = jnp.where(allowed, scores * score_scale, -1000000000.0)
            top = jnp.max(scores, axis=-1, keepdims=True)
            e = jnp.exp(scores - top)
            weights = (e * (1.0 / jnp.sum(e, axis=-1, keepdims=True))).astype(bf16)
            out = dot(weights, v)
            mix[:, at : at + 2 * HEAD] = jnp.where(low, out[:rows], out[rows:]).astype(bf16)

        mixture = mix[...]
        per = SECTIONS // CHUNKS
        for k in range(1, group):
            part = lax.rem(me + k, group)
            for z in range(SECTIONS):
                ref = sends[(k - 1) * CHUNKS + z // per]
                column = rows_of(z, part, group, share)
                at = (z % per) * share
                ref[:, at : at + share] = dot(mixture, wo[:, column]).astype(bf16)


def tail_kernel(group, t, batches, mix, *refs):
    _, me, active = position(group, t, batches)
    xq = refs[:CHUNKS]
    wo = refs[CHUNKS]
    bases = refs[CHUNKS + 1 :]
    share = wo.shape[1] // (group * SECTIONS)

    @pl.when(active)
    def _():
        mixture = mix[...]
        per = SECTIONS // CHUNKS
        for z in range(SECTIONS):
            column = rows_of(z, me, group, share)
            at = (z % per) * share
            res = xq[z // per][:, at : at + share].astype(f32)
            bases[z // per][:, at : at + share] = dot(mixture, wo[:, column]) + res


def hold_weights(w_in, w_out):
    w_in = pltpu.with_memory_space_constraint(w_in, pltpu.VMEM)
    w_out = pltpu.with_memory_space_constraint(w_out, pltpu.VMEM)

    def touch(a_ref, out):
        out[...] = jnp.zeros_like(out)

    token = pl.pallas_call(
        touch,
        out_shape=jax.ShapeDtypeStruct((8, 128), f32),
        in_specs=[VMEM],
        out_specs=VMEM,
        compiler_params=params(1 << 20),
        name="touch",
    )(w_in)
    return w_in, w_out, token


def relay(
    src_embed, tgt_embed, src_lengths, tgt_lengths, attn_in, attn_out, norm_gain, final_gain
):
    axis = "segment"
    segments = lax.axis_size(axis)
    group = segments // SECTIONS
    index = lax.axis_index(axis).astype(jnp.uint32)
    section = lax.div(index, jnp.uint32(group)).astype(jnp.int32)
    member = lax.rem(index, jnp.uint32(group)).astype(jnp.int32)
    at_section = [section == p for p in range(SECTIONS)]
    section, member, at_section = lax.optimization_barrier((section, member, at_section))
    batches, rows, share = src_embed.shape
    part_width = SECTIONS * share
    chunk_width = part_width // CHUNKS
    w_in = attn_in[0]
    w_out = attn_out[0]
    head_cols = w_out.shape[0]
    gain_q = norm_gain[:1]
    for p in range(1, SECTIONS):
        gain_q = jnp.where(at_section[p], norm_gain[p : p + 1], gain_q)
    gain_kv = jnp.where(at_section[2], final_gain[None], gain_q)

    def permute(value, pairs):
        return lax.ppermute(value, axis, pairs)

    def partners(k, sections=range(SECTIONS)):
        return [
            (p * group + q, p * group + (q + k) % group)
            for p in sections
            for q in range(group)
        ]

    def onward(k, sections):
        return [
            (p * group + q, (p + 1) * group + (q + k) % group)
            for p in sections
            if p < SECTIONS - 1
            for q in range(group)
        ]

    def shift_pairs(by):
        return [
            (((0 if first else 2) + by) % SECTIONS * group + q, (0 if first else 2) * group + q)
            for first in (True, False)
            for q in range(group)
        ]

    def collect(low, high):
        source = src_embed[low:high]
        target = tgt_embed[low:high]
        payloads = [jnp.where(at_section[by], source, target) for by in range(SECTIONS)]
        payloads = lax.optimization_barrier(payloads)
        pieces = {0: payloads[0]}
        for by in range(1, SECTIONS):
            pieces[by] = permute(payloads[by], shift_pairs(by))
        return pieces

    def part_of(pieces, at):
        rotated = [pieces[by][at] for by in range(SECTIONS)]
        ordered = []
        for z in range(SECTIONS):
            value = rotated[z]
            other = rotated[(z - 2) % SECTIONS]
            ordered.append(jnp.where(at_section[0], value, other))
        width = chunk_width // share
        return [
            jnp.concatenate(ordered[c * width : (c + 1) * width], -1) for c in range(CHUNKS)
        ]

    periods = batches + SECTIONS - 1
    lens = jnp.concatenate([src_lengths, tgt_lengths]).astype(jnp.int32)
    lens = jnp.broadcast_to(lens[:, None], (2 * batches, rows))

    early = collect(0, 1)
    late = [collect(1, batches)]
    w_in, w_out, token = hold_weights(w_in, w_out)
    entry = {}

    def enter(b):
        mine = part_of(early, 0) if b == 0 else part_of(late[0], b - 1)
        mine = lax.optimization_barrier(mine)
        parts = [mine]
        for k in range(1, group):
            parts.append([permute(v, partners(k, (0, 2))) for v in mine])
        entry[b] = parts


    def flat(lists):
        return [v for inner in lists for v in inner]

    def gated(values, gate):
        return lax.optimization_barrier((values, gate))[0]

    def merge(at, ours, theirs):
        return [
            [jnp.where(at_section[at], a, c) for a, c in zip(ra, rc)]
            for ra, rc in zip(ours, theirs)
        ]

    def feed(t, came):
        def select(rows):
            xk = None if came is None else came[rows]
            if t < batches:
                mine = entry[t][rows]
                xk = mine if xk is None else merge(0, mine, xk)
            xq = xk
            if 0 <= t - 2 < batches:
                xq = merge(2, entry[t - 2][rows], xk)
            return xk, xq

        xk, xq = select(slice(0, 1))
        partial = own((t, xk, xq), token)
        if came is not None:
            came = came[:1] + gated(came[1:], partial[1])
        more_k, more_q = select(slice(1, None))
        same = xq is xk
        xk = xk + more_k
        return (t, xk, xk if same else xq + more_q), partial

    def own(fed, after):
        t, xk, xq = fed
        same = xq is xk
        inputs = list(xk[0]) + ([] if same else list(xq[0]))
        return pl.pallas_call(
            functools.partial(own_kernel, group, same, t, batches),
            out_shape=(
                jax.ShapeDtypeStruct((rows, 3 * head_cols), f32),
                jax.ShapeDtypeStruct((rows, 256), f32),
            ),
            in_specs=[VMEM, ANY] + [VMEM] * (len(inputs) + 3),
            out_specs=(VMEM, VMEM),
            compiler_params=params(2 << 20),
            cost_estimate=pl.CostEstimate(
                flops=2 * rows * part_width * 3 * head_cols,
                bytes_accessed=1 << 20,
                transcendentals=0,
            ),
            name="own",
        )(lens, after, *inputs, gain_q, gain_kv, w_in)

    n_send = CHUNKS * (group - 1)

    def rest(fed, partial, after):
        t, xk, xq = fed
        same = xq is xk
        inputs = flat(xk[1:]) + ([] if same else flat(xq[1:]))
        outs = pl.pallas_call(
            functools.partial(rest_kernel, group, same, t, batches),
            out_shape=tuple(
                [jax.ShapeDtypeStruct((rows, chunk_width), bf16)] * n_send
                + [jax.ShapeDtypeStruct((rows, head_cols), bf16)]
            ),
            in_specs=[VMEM, ANY] + [VMEM] * (len(inputs) + 6),
            out_specs=tuple([VMEM] * (n_send + 1)),
            scratch_shapes=[pltpu.VMEM((rows, 3 * head_cols), bf16)],
            compiler_params=params(4 << 20),
            cost_estimate=pl.CostEstimate(
                flops=4 * rows * part_width * 3 * head_cols,
                bytes_accessed=1 << 20,
                transcendentals=rows * rows * (head_cols // HEAD),
            ),
            name="rest",
        )(lens, after, *inputs, gain_q, gain_kv, w_in, w_out, *partial)
        return outs[:n_send], outs[n_send]

    def tail(fed, mix):
        t, _, xq = fed
        return pl.pallas_call(
            functools.partial(tail_kernel, group, t, batches),
            out_shape=tuple([jax.ShapeDtypeStruct((rows, chunk_width), f32)] * CHUNKS),
            in_specs=[VMEM] * (2 + CHUNKS),
            out_specs=tuple([VMEM] * CHUNKS),
            compiler_params=params(1 << 20),
            cost_estimate=pl.CostEstimate(
                flops=2 * rows * part_width * head_cols, bytes_accessed=1 << 20, transcendentals=0
            ),
            name="tail",
        )(mix, *xq[0], w_out)

    enter(0)
    fed, partial = feed(0, None)
    finals = {}
    exits = []

    def leave(slots):
        pieces = []
        for z in range(SECTIONS):
            at, offset = divmod(z * share, chunk_width)
            piece = jnp.stack([finals[b][at][:, offset : offset + share] for b in slots])
            if z < SECTIONS - 1:
                pairs = [((SECTIONS - 1) * group + q, z * group + q) for q in range(group)]
                piece = permute(piece, pairs)
            pieces.append(piece)
        result = pieces[-1]
        for z in range(SECTIONS - 1):
            result = jnp.where(at_section[z], pieces[z], result)
        exits.append(result)

    for t in range(periods):
        live = [p for p in range(SECTIONS) if 0 <= t - p < batches]
        sends, mix = rest(fed, partial, token)
        bases = tail(fed, mix)
        taken = [
            [permute(sends[(k - 1) * CHUNKS + c], partners(k)) for k in range(1, group)]
            for c in range(CHUNKS)
        ]
        if 0 < t < batches - 1:
            enter(t + 1)
        if t + 1 == periods and batches > 1:
            leave(range(batches - 1))
        came = [[None] * CHUNKS for _ in range(group)]
        done = []
        for c in range(CHUNKS):
            total = bases[c]
            for v in taken[c]:
                total = total + v.astype(f32)
            total = total.astype(bf16)
            done.append(total)
            if t + 1 < periods:
                for k in range(group):
                    came[k][c] = permute(total, onward(k, live))
        if t == 0:
            late[0] = gated(late[0], done)
            enter(1)
        if t >= SECTIONS - 1:
            finals[t - SECTIONS + 1] = done
        if t + 1 < periods:
            fed, partial = feed(t + 1, came)
    leave(range(batches - 1, batches))
    return jnp.concatenate(exits)


def solution(mesh):
    in_specs = (
        P("dp", None, "segment"),
        P("dp", None, "segment"),
        P("dp"),
        P("dp"),
        P("segment", None, None),
        P("segment", None, None),
        P(),
        P(),
    )
    out_specs = P("dp", None, "segment")
    return jax.shard_map(relay, mesh=mesh, in_specs=in_specs, out_specs=out_specs, check_vma=False)
```
